128 devices in a mesh: expert: 4 (over x), shard: 32 (over z, y, core).
Axes of the slice: x: 4, y: 4, z: 4, core: 2. Of those that a mesh axis runs over, the one named last changes fastest.
Arguments:
- hidden: bfloat16 [256, 4096], P('shard'), may hold values from -6 to 6
- queries: bfloat16 [256, 32, 128], P('shard', 'expert'), may hold values from -30 to 30
- key_cache: bfloat16 [256, 512, 8, 128], P('shard', None, 'expert'), may hold values from -16 to 16
- value_cache: bfloat16 [256, 512, 8, 128], P('shard', None, 'expert'), may hold values from -6 to 6
- out_weight: bfloat16 [4096, 4096], P('expert', 'shard'), may hold values from -0.09375 to 0.09375
- norm_gain: bfloat16 [4096], replicated, may hold values from 0.099609375 to 1.8984375
- router: bfloat16 [4096, 8], replicated, may hold values from -0.09375 to 0.09375
- expert_ids: int32 [256, 2], replicated, may hold values from 0 to 7, all different within a row; in each aligned block of 256 rows (0 to 255, 256 to 511, ...) at most 128 rows name the same one
- gate_weight: bfloat16 [8, 4096, 14336], P('expert', None, 'shard'), may hold values from -0.09375 to 0.09375
- up_weight: bfloat16 [8, 4096, 14336], P('expert', None, 'shard'), may hold values from -0.09375 to 0.09375
- down_weight: bfloat16 [8, 14336, 4096], P('expert', 'shard'), may hold values from -0.046875 to 0.046875
Outputs:
- layer_out: bfloat16 [256, 4096], P('shard')
The draws below stay inside these ranges and needn't reach their ends.
Inputs may be any that keep to these rules, and one draw needn't show every extreme that they name: `expert_ids`: each token names two different experts; over all 256 tokens no expert is named by more than 128 tokens, a bound that some block reaches.
All inputs are finite; a program needn't handle non-finite values.
Results may differ from the reference program's by a relative error of at most 0.008.
Values may be sent and summed in bfloat16 or wider, within the bound.
No kernel may reach another device: no remote copies, remote signals or barrier semaphores. Data moves between devices by JAX's collectives and lax.ppermute only.
A program may use at most 128 MiB of HBM per device.

```python
import math
import jax
import jax.numpy as jnp
import numpy as np
from jax import lax

D = 4096
FF = 14336
EXPERTS = 8
HEADS = 32
KV_HEADS = 8
HD = 128
POS = 512
TOKENS = 256
CAP = 128


def shared_attention(key):
    base_key = jax.random.fold_in(key, 7)
    key_query, key_rows = jax.random.split(base_key, 2)
    query_draw = jnp.clip(jax.random.normal(key_query, (TOKENS, HEADS, HD), jnp.float32), -4.0, 4.0)
    key_draw = jnp.clip(jax.random.normal(key_rows, (TOKENS, POS, KV_HEADS, HD), jnp.float32), -4.0, 4.0)
    return (query_draw, key_draw)


def draw_queries(key, part):
    return shared_attention(key)[0].astype(jnp.bfloat16)


def draw_key_cache(key, part):
    return shared_attention(key)[1].astype(jnp.bfloat16)


def levels(key, dims, cuts, smallest, high):
    def one(axis_at, shards_of):
        heights = jax.random.uniform(jax.random.fold_in(jax.random.fold_in(key, 6), axis_at), (shards_of,), jnp.float32, smallest / len(cuts), high / len(cuts))
        return jnp.repeat(jnp.exp(heights), dims[axis_at] // shards_of).reshape((-1,) + (1,) * (len(dims) - axis_at - 1))

    factor_of = one(*cuts[0])
    for cut in cuts[1:]:
        factor_of = factor_of * one(*cut)
    return factor_of


def routed_block(stream_key, own, number, rows, amount, top, most, skew):
    sequence = jax.random.permutation(stream_key, amount)
    packed, common = shares(amount, rows * top, most, skew, True), shares(amount, rows * top, most, skew, False)
    places = jnp.arange(amount)

    def named(tallies, rotation):
        used = int((tallies > 0).sum())
        fixed = max(1, used // 4)
        shifted = fixed + (places - fixed + rotation * (used - fixed)) % max(1, amount - fixed)
        return jnp.zeros((amount,), jnp.int32).at[sequence[jnp.where(places < fixed, places, shifted)]].set(jnp.asarray(tallies, jnp.int32))

    tallies = jnp.where(number % 4 == 0, named(packed, number // 4), named(common, number - number // 4 - 1))
    mixed = jax.random.permutation(jax.random.fold_in(own, 3), amount)
    source_of, sink = mixed[0:amount // 2 * 2:2], mixed[1:amount // 2 * 2:2]
    margin = jnp.minimum(tallies[source_of] - 1, most - tallies[sink]) // 2
    margin = jnp.where((source_of == sequence[0]) | (sink == sequence[0]) | (tallies[sink] == 0), 0, jnp.maximum(margin, 0))
    shifted = jax.random.randint(jax.random.fold_in(own, 4), (amount // 2,), 0, 1 << 20) % (margin + 1)
    tallies = tallies.at[source_of].add(-shifted).at[sink].add(shifted)
    items = jnp.searchsorted(jnp.cumsum(tallies), jnp.arange(rows * top), side="right").astype(jnp.int32)
    table = items.reshape(top, rows).T
    table = table[jax.random.permutation(jax.random.fold_in(own, 1), rows)]
    rotation = jax.random.randint(jax.random.fold_in(own, 2), (rows, 1), 0, top)
    return jnp.take_along_axis(table, (jnp.arange(top)[None, :] + rotation) % top, axis=1)


def shares(count, total, most, lean, full):
    portions = [(1 << 20) // math.isqrt(grade ** lean) + 1 for grade in range(1, count + 1)]
    largest = most if full else min(most, max(-(-total // count), total * portions[0] // sum(portions)))
    least = 1 if total - largest >= count - 1 else 0
    counts, surplus = [largest] + [least] * (count - 1), total - largest - least * (count - 1)
    while surplus > 0:
        candidates = [i for i in range(1, count) if counts[i] < largest] or [i for i in range(1, count) if counts[i] < most]
        mass, budget = sum([portions[i] for i in candidates]), surplus
        for i in candidates:
            extra = min(most - counts[i], max(1, budget * portions[i] // mass), surplus)
            counts[i] = counts[i] + extra
            surplus = surplus - extra
    return np.array(counts)


def gaussian(stream_key, dims, spread, limit, cuts=(), held_as=jnp.bfloat16):
    values = spread * jax.random.normal(stream_key, dims, jnp.float32)
    if cuts:
        values = values * levels(stream_key, dims, cuts, -0.22, 0.18)
    return jnp.clip(values, -limit, limit).astype(held_as)


def setup_inputs(seed: int = 0) -> dict:
    key_list = jax.random.split(jax.random.key(seed), 12)
    hidden = gaussian(key_list[0], (TOKENS, D), 1.0, 6.0, ((0, 32),))
    queries = draw_queries(jax.random.fold_in(key_list[11], 71), 0)
    key_cache = draw_key_cache(jax.random.fold_in(key_list[11], 71), 0)
    value_cache = gaussian(key_list[3], (TOKENS, POS, KV_HEADS, HD), 1.0, 6.0, ((0, 32), (2, 4)))
    out_weight = gaussian(key_list[4], (HEADS * HD, D), (HEADS * HD) ** -0.5, 0.09375, ((0, 4), (1, 32)))
    norm_gain = jnp.clip(1.0 + 0.18 * jax.random.normal(key_list[5], (D,), jnp.float32), 0.099609375, 1.8984375).astype(jnp.bfloat16)
    router = gaussian(key_list[6], (D, EXPERTS), D ** -0.5, 0.09375)
    expert_ids_keys = jax.random.split(jax.random.fold_in(key_list[7], 1), TOKENS // TOKENS)
    expert_ids_turns = jax.random.permutation(jax.random.fold_in(key_list[7], 3), TOKENS // TOKENS)
    expert_ids = jax.vmap(lambda own, number: routed_block(jax.random.fold_in(key_list[7], 2), own, number, TOKENS, EXPERTS, 2, CAP, 2))(expert_ids_keys, expert_ids_turns).reshape((TOKENS, 2))
    gate_weight = gaussian(key_list[8], (EXPERTS, D, FF), D ** -0.5, 0.09375, ((0, 4), (2, 32)))
    up_weight = gaussian(key_list[9], (EXPERTS, D, FF), D ** -0.5, 0.09375, ((0, 4), (2, 32)))
    down_weight = gaussian(key_list[10], (EXPERTS, FF, D), FF ** -0.5, 0.046875, ((0, 4), (1, 32)))
    return {"hidden": hidden, "queries": queries, "key_cache": key_cache, "value_cache": value_cache, "out_weight": out_weight, "norm_gain": norm_gain, "router": router, "expert_ids": expert_ids, "gate_weight": gate_weight, "up_weight": up_weight, "down_weight": down_weight}


def reference(hidden, queries, key_cache, value_cache, out_weight, norm_gain, router, expert_ids, gate_weight, up_weight, down_weight):
    per_kv = HEADS // KV_HEADS
    query_blocks = queries.astype(jnp.float32).reshape(TOKENS, KV_HEADS, per_kv, HD)
    scores = jnp.einsum('tkgd,tpkd->tkgp', query_blocks, key_cache.astype(jnp.float32)) / math.sqrt(HD)
    attn_weights = jax.nn.softmax(scores, axis=-1).astype(jnp.bfloat16)
    attended = jnp.einsum('tkgp,tpkd->tkgd', attn_weights.astype(jnp.float32), value_cache.astype(jnp.float32))
    attended = attended.astype(jnp.bfloat16).reshape(TOKENS, HEADS * HD)
    stream = hidden.astype(jnp.float32) + jnp.dot(attended, out_weight, preferred_element_type=jnp.float32)
    scaled = stream * lax.rsqrt(lax.optimization_barrier(jnp.mean(stream * stream, axis=-1, keepdims=True)) + 1e-05)
    normed = (scaled * norm_gain.astype(jnp.float32)).astype(jnp.bfloat16)
    logits = jnp.dot(normed, router, preferred_element_type=jnp.float32)
    top_first = jnp.take_along_axis(logits, expert_ids[:, 0:1], axis=1)[:, 0]
    top_second = jnp.take_along_axis(logits, expert_ids[:, 1:2], axis=1)[:, 0]
    weight_first = 1.0 / (1.0 + jnp.exp(top_second - top_first))
    weight_second = 1.0 / (1.0 + jnp.exp(top_first - top_second))

    def expert_step(summed, expert):
        gated = jnp.dot(normed, gate_weight[expert], preferred_element_type=jnp.float32)
        upward = jnp.dot(normed, up_weight[expert], preferred_element_type=jnp.float32)
        activated = (jax.nn.silu(gated) * upward).astype(jnp.bfloat16)
        expert_out = jnp.dot(activated, down_weight[expert], preferred_element_type=jnp.float32)
        routed_weight = jnp.where(expert_ids[:, 0] == expert, weight_first, 0.0) + jnp.where(expert_ids[:, 1] == expert, weight_second, 0.0)
        return (summed + routed_weight[:, None] * expert_out, None)
    start_sum = jnp.zeros((TOKENS, D), jnp.float32)
    expert_mix, _ = lax.scan(expert_step, start_sum, jnp.arange(EXPERTS, dtype=jnp.int32))
    return (stream + expert_mix).astype(jnp.bfloat16)
```

```python
import functools
import math

import jax
import jax.numpy as jnp
from jax import lax
from jax.experimental import pallas as pl
from jax.experimental.pallas import tpu as pltpu
from jax.sharding import Mesh
from jax.sharding import PartitionSpec as P

SHARD = ("shard_0", "shard_1", "shard_2")
PLANE = ("shard_0", "shard_1")
CORE_MAJOR = ("shard_2", "shard_0", "shard_1")
F32 = jnp.float32
BF16 = jnp.bfloat16


def shifted(x, axis, by):
    size = lax.axis_size(axis)
    return lax.ppermute(x, axis, [(i, (i + by) % size) for i in range(size)])


def sum_over_groups(part):
    one, two, three = (shifted(part, "expert", by) for by in (1, 2, 3))
    return (part.astype(F32) + two.astype(F32)) + (one.astype(F32) + three.astype(F32))


def expert_kernel(
    place, own, partner, ids, gain, router, attn, gate, up, down,
    send, keep, weights, down_v, mixed, hidden_t, act, sems,
):
    core, shard, first_expert, adds = place[0], place[1], place[2], place[3]
    units = gate.shape[0]
    half_units = units // 2
    tokens = own.shape[2]
    half = tokens // 2
    width = down.shape[1]
    block = own.shape[1]
    copies = [
        pltpu.make_async_copy(
            source.at[pl.ds(m * half_units, half_units)],
            weights.at[pl.ds(at + m * half_units, half_units)],
            sems.at[number * 2 + m],
        )
        for number, (source, at) in enumerate(((gate, 0), (up, units)))
        for m in range(2)
    ]
    copies = [copies[0], copies[2], copies[1], copies[3]]
    last = pltpu.make_async_copy(down, down_v, sems.at[4])
    for copy in copies:
        copy.start()
    last.start()

    def norm_block(j, squares):
        for mine, part in ((core, own), (1 - core, partner)):
            x = part[j]
            rows = pl.ds(pl.multiple_of((2 * j + mine) * block, block), block)
            g = gain[rows, :]
            mixed[rows, :] = (
                x.astype(F32) * jnp.concatenate([g, g], axis=1).astype(F32)
            ).astype(BF16)
            y = x.astype(F32)
            squares = squares + (y * y).reshape(block // 8, 8, tokens).sum(axis=0)
        return squares

    squares = lax.fori_loop(0, own.shape[0], norm_block, jnp.zeros((8, tokens), F32))
    scale = lax.rsqrt(squares.sum(axis=0, keepdims=True) / width + 1e-05)
    logits = jnp.dot(router[...], mixed[...], preferred_element_type=F32) * scale
    numbers = lax.broadcasted_iota(jnp.int32, logits.shape, 0)
    first, second = ids[0:1, :], ids[1:2, :]
    a = jnp.where(numbers == first, logits, 0.0).sum(axis=0, keepdims=True)
    b = jnp.where(numbers == second, logits, 0.0).sum(axis=0, keepdims=True)
    weight_first = 1.0 / (1.0 + jnp.exp(b - a))
    weight_second = 1.0 / (1.0 + jnp.exp(a - b))

    for at, copy in zip((0, units, half_units, units + half_units), copies):
        copy.wait()
        hidden_t[pl.ds(at, half_units), :] = jnp.dot(
            weights[pl.ds(at, half_units), :], mixed[...], preferred_element_type=F32
        )

    for m in range(2):
        expert = first_expert + m
        routed = jnp.where(first == expert, weight_first, 0.0) + jnp.where(
            second == expert, weight_second, 0.0
        )
        gated = hidden_t[pl.ds(m * half_units, half_units), :] * scale
        upward = hidden_t[pl.ds(units + m * half_units, half_units), :] * scale
        value = gated / (1.0 + jnp.exp(-gated)) * upward * routed
        turned = value.T.astype(BF16)
        for h in range(2):
            rows = pl.ds(pl.multiple_of(jnp.where(core == h, half, 0), half), half)
            act[m, rows, :] = turned[h * half : (h + 1) * half, :]

    last.wait()
    step = 512

    def down_block(n, carry):
        columns = pl.ds(pl.multiple_of(n * step, step), step)
        total = jnp.dot(
            act[0], down_v[pl.ds(0, half_units), columns], preferred_element_type=F32
        ) + jnp.dot(
            act[1], down_v[pl.ds(half_units, half_units), columns], preferred_element_type=F32
        )
        send[:, columns] = total[:half].astype(BF16)
        keep[:, columns] = total[half:]
        return carry

    lax.fori_loop(0, width // step, down_block, 0)
    rows = attn[...].T * adds.astype(F32)
    columns = pl.ds(pl.multiple_of(shard * block, block), block)
    theirs = jnp.where(core == 0, rows[half:], rows[:half])
    mine = jnp.where(core == 0, rows[:half], rows[half:])
    keep[:, columns] += mine
    send[:, columns] = (send[:, columns].astype(F32) + theirs).astype(BF16)


def experts(place, own, partner, ids, gain, router, attn, gate, up, down):
    units, width = down.shape
    tokens = own.shape[2]
    vmem = pl.BlockSpec(memory_space=pltpu.VMEM)
    hbm = pl.BlockSpec(memory_space=pl.ANY)
    return pl.pallas_call(
        expert_kernel,
        out_shape=(
            jax.ShapeDtypeStruct((tokens // 2, width), BF16),
            jax.ShapeDtypeStruct((tokens // 2, width), F32),
        ),
        in_specs=[pl.BlockSpec(memory_space=pltpu.SMEM)] + [vmem] * 6 + [hbm] * 3,
        out_specs=(vmem, vmem),
        scratch_shapes=[
            pltpu.VMEM((2 * units, width), BF16),
            pltpu.VMEM((units, width), BF16),
            pltpu.VMEM((width, tokens), BF16),
            pltpu.VMEM((2 * units, tokens), F32),
            pltpu.VMEM((2, tokens, units // 2), BF16),
            pltpu.SemaphoreType.DMA((5,)),
        ],
        compiler_params=pltpu.CompilerParams(vmem_limit_bytes=60 * 1024 * 1024),
        cost_estimate=pl.CostEstimate(
            flops=6 * tokens * units * width,
            bytes_accessed=6 * units * width,
            transcendentals=2 * units * tokens,
        ),
        name="experts",
    )(place, own, partner, ids, gain, router, attn, gate, up, down)


def on_device(
    hidden, queries, key_cache, value_cache, out_weight, norm_gain, router,
    expert_ids, gate_weight, up_weight, down_weight,
):
    count_local, heads_local, head_size = queries.shape
    kv_local = key_cache.shape[2]
    width = hidden.shape[1]
    block = out_weight.shape[1]
    chips, cores = lax.axis_size(PLANE), lax.axis_size("shard_2")
    shards = chips * cores
    tokens = shards * count_local
    query_blocks = queries.reshape(count_local, kv_local, heads_local // kv_local, head_size)
    scores = jnp.einsum(
        "tkgd,tpkd->tkgp", query_blocks, key_cache, preferred_element_type=F32
    ) / math.sqrt(head_size)
    attn_weights = jax.nn.softmax(scores, axis=-1).astype(BF16)
    attended = jnp.einsum(
        "tkgp,tpkd->tkgd", attn_weights, value_cache, preferred_element_type=F32
    )
    attended = attended.astype(BF16).reshape(count_local, heads_local * head_size)
    own_cols = hidden.reshape(count_local, chips, cores, block).transpose(2, 1, 0, 3)
    pieces = jnp.concatenate(
        [
            jnp.broadcast_to(attended[None], (shards, *attended.shape)),
            own_cols.reshape(shards, count_local, block),
        ],
        axis=-1,
    )
    arrived = lax.all_to_all(pieces, CORE_MAJOR, 0, 0, tiled=True).reshape(tokens, -1)
    heads = attended.shape[1]
    part = lax.dot_general(
        out_weight, arrived[:, :heads], (((0,), (1,)), ((), ())), preferred_element_type=F32
    ).astype(BF16)
    hidden_t = arrived[:, heads:].T.astype(F32)
    attn_out = sum_over_groups(part)
    stream = (attn_out + hidden_t).astype(BF16)
    own = lax.all_to_all(
        jnp.broadcast_to(stream[None], (chips, block, tokens)), PLANE, 0, 0, tiled=True
    )
    partner = shifted(own, "shard_2", 1)
    core = lax.axis_index("shard_2")
    shard = lax.axis_index(PLANE) * cores + core
    group = lax.axis_index("expert")
    local = gate_weight.shape[0]
    place = jnp.stack([core, shard, group * local, (group == 0).astype(jnp.int32)]).astype(jnp.int32)
    ids = expert_ids.reshape(chips, cores, count_local, 2).transpose(3, 1, 0, 2).reshape(2, tokens)
    units = local * gate_weight.shape[2]
    send, keep = experts(
        place,
        own,
        partner,
        ids,
        jnp.broadcast_to(norm_gain[:, None], (width, 128)),
        router.T,
        attn_out,
        gate_weight.transpose(0, 2, 1).reshape(units, width),
        up_weight.transpose(0, 2, 1).reshape(units, width),
        down_weight.reshape(units, width),
    )
    pair = (keep + shifted(send, "shard_2", 1).astype(F32)).astype(BF16)
    parts = lax.all_to_all(pair.reshape(chips, count_local, width), PLANE, 0, 0, tiled=True)
    reduced = parts.astype(F32).sum(axis=0).astype(BF16)
    return (hidden.astype(F32) + sum_over_groups(reduced)).astype(BF16)


def solution(mesh):
    split = Mesh(
        mesh.devices.reshape(mesh.shape["expert"], 4, 4, 2),
        ("expert", "shard_0", "shard_1", "shard_2"),
    )
    in_specs = (
        P(SHARD, None),
        P(SHARD, "expert", None),
        P(SHARD, None, "expert", None),
        P(SHARD, None, "expert", None),
        P("expert", SHARD),
        P(),
        P(),
        P(),
        P("expert", None, SHARD),
        P("expert", None, SHARD),
        P("expert", SHARD, None),
    )
    return jax.shard_map(
        on_device, mesh=split, in_specs=in_specs, out_specs=P(SHARD, None), check_vma=False
    )
```

```python
import math

import jax
import jax.numpy as jnp
from jax import lax
from jax.experimental import pallas as pl
from jax.experimental.pallas import tpu as pltpu
from jax.sharding import Mesh
from jax.sharding import PartitionSpec as P

SHARD = ("shard_0", "shard_1", "shard_2")
PLANE = ("shard_0", "shard_1")
F32 = jnp.float32
BF16 = jnp.bfloat16


def shifted(x, axis, by):
    size = lax.axis_size(axis)
    return lax.ppermute(x, axis, [(i, (i + by) % size) for i in range(size)])


def sum_over_groups(part, ready=()):
    others = tuple(shifted(part, "expert", by) for by in (1, 2, 3))
    (one, two, three), ready = lax.optimization_barrier((others, ready))
    total = (part.astype(F32) + two.astype(F32)) + (one.astype(F32) + three.astype(F32))
    return (total, ready) if ready else total


def expert_kernel(
    place, own, partner, ids, gain, router, attn, gate_hbm, up_hbm, down_hbm,
    send, keep, mixed, hidden_t, act, gate_up, down, sems,
):
    core, shard, first_expert, adds = place[0], place[1], place[2], place[3]
    units, width = down.shape
    half_units = units // 2
    block, tokens = own.shape[1:]
    half = tokens // 2
    parts = sems.shape[0] - 4
    step = width // parts

    def gate_up_copy(k, source, at):
        return pltpu.make_async_copy(
            source.at[pl.ds(at, half_units)], gate_up.at[k], sems.at[k]
        )

    def down_copy(n):
        columns = pl.ds(pl.multiple_of(n * step, step), step)
        return pltpu.make_async_copy(
            down_hbm.at[:, columns], down.at[:, columns], sems.at[4 + n]
        )

    for m in range(2):
        gate_up_copy(2 * m, gate_hbm, m * half_units).start()
        gate_up_copy(2 * m + 1, up_hbm, m * half_units).start()
    for n in range(parts):
        down_copy(n).start()

    def norm_block(j, squares):
        for mine, part in ((core, own), (1 - core, partner)):
            x = part[j]
            if part is partner:
                x = jnp.concatenate([x[:, half:], x[:, :half]], axis=1)
            rows = pl.ds(pl.multiple_of((2 * j + mine) * block, block), block)
            g = gain[rows, :]
            y = x.astype(F32)
            mixed[rows, :] = (y * jnp.concatenate([g, g], axis=1).astype(F32)).astype(BF16)
            squares = squares + (y * y).reshape(block // 8, 8, tokens).sum(axis=0)
        return squares

    squares = lax.fori_loop(0, own.shape[0], norm_block, jnp.zeros((8, tokens), F32))
    scale = lax.rsqrt(squares.sum(axis=0, keepdims=True) / width + 1e-05)
    logits = jnp.dot(router[...], mixed[...], preferred_element_type=F32) * scale
    numbers = lax.broadcasted_iota(jnp.int32, logits.shape, 0)
    named = ids[...]
    named = jnp.where(
        core == 0, named, jnp.concatenate([named[:, half:], named[:, :half]], axis=1)
    )
    first, second = named[0:1, :], named[1:2, :]
    a = jnp.where(numbers == first, logits, 0.0).sum(axis=0, keepdims=True)
    b = jnp.where(numbers == second, logits, 0.0).sum(axis=0, keepdims=True)
    weight_first = 1.0 / (1.0 + jnp.exp(b - a))
    weight_second = 1.0 / (1.0 + jnp.exp(a - b))

    def gate_up_part(k, carry):
        gate_up_copy(k, gate_hbm, 0).wait()
        hidden_t[k] = jnp.dot(gate_up[k], mixed[...], preferred_element_type=F32)
        return carry

    lax.fori_loop(0, 4, gate_up_part, 0)
    for m in range(2):
        expert = first_expert + m
        routed = jnp.where(first == expert, weight_first, 0.0) + jnp.where(
            second == expert, weight_second, 0.0
        )
        gated = hidden_t[2 * m] * scale
        upward = hidden_t[2 * m + 1] * scale
        value = gated / (1.0 + jnp.exp(-gated)) * upward * routed
        act[m] = value.T.astype(BF16)

    def down_part(n, carry):
        down_copy(n).wait()
        columns = pl.ds(pl.multiple_of(n * step, step), step)
        total = jnp.dot(
            act[0], down[pl.ds(0, half_units), columns], preferred_element_type=F32
        ) + jnp.dot(
            act[1], down[pl.ds(half_units, half_units), columns], preferred_element_type=F32
        )
        keep[:, columns] = total[:half].astype(BF16)
        send[:, columns] = total[half:].astype(BF16)
        return carry

    lax.fori_loop(0, parts, down_part, 0)
    rows = attn[...].astype(F32).T * adds.astype(F32)
    columns = pl.ds(pl.multiple_of(shard * block, block), block)
    keep[:, columns] = (keep[:, columns].astype(F32) + rows[:half]).astype(BF16)
    send[:, columns] = (send[:, columns].astype(F32) + rows[half:]).astype(BF16)


def experts(place, own, partner, ids, gain, router, attn, gate, up, down):
    units, width = down.shape
    tokens = own.shape[2]
    vmem = pl.BlockSpec(memory_space=pltpu.VMEM)
    hbm = pl.BlockSpec(memory_space=pl.ANY)
    half = jax.ShapeDtypeStruct((tokens // 2, width), BF16)
    return pl.pallas_call(
        expert_kernel,
        out_shape=(half, half),
        in_specs=[pl.BlockSpec(memory_space=pltpu.SMEM)] + [vmem] * 6 + [hbm] * 3,
        out_specs=(vmem, vmem),
        scratch_shapes=[
            pltpu.VMEM((width, tokens), BF16),
            pltpu.VMEM((4, units // 2, tokens), F32),
            pltpu.VMEM((2, tokens, units // 2), BF16),
            pltpu.VMEM((4, units // 2, width), BF16),
            pltpu.VMEM((units, width), BF16),
            pltpu.SemaphoreType.DMA((8,)),
        ],
        compiler_params=pltpu.CompilerParams(vmem_limit_bytes=48 * 1024 * 1024),
        cost_estimate=pl.CostEstimate(
            flops=6 * tokens * units * width,
            bytes_accessed=6 * units * width,
            transcendentals=2 * units * tokens,
        ),
        name="experts",
    )(place, own, partner, ids, gain, router, attn, gate, up, down)


def on_device(
    hidden, queries, key_cache, value_cache, out_weight, norm_gain, router,
    expert_ids, gate_weight, up_weight, down_weight,
):
    count_local, heads_local, head_size = queries.shape
    kv_local = key_cache.shape[2]
    width = hidden.shape[1]
    block = out_weight.shape[1]
    chips, cores = lax.axis_size(PLANE), lax.axis_size("shard_2")
    tokens = chips * cores * count_local
    core = lax.axis_index("shard_2")
    shard = lax.axis_index(PLANE) * cores + core
    group = lax.axis_index("expert")
    query_blocks = queries.reshape(count_local, kv_local, heads_local // kv_local, head_size)
    scores = jnp.einsum(
        "tkgd,tpkd->tkgp", query_blocks, key_cache, preferred_element_type=F32
    ) / math.sqrt(head_size)
    attn_weights = jax.nn.softmax(scores, axis=-1).astype(BF16)
    attended = jnp.einsum(
        "tkgp,tpkd->tkgd", attn_weights, value_cache, preferred_element_type=F32
    )
    heads = heads_local * head_size
    attended = attended.astype(BF16).reshape(count_local, heads)
    pieces = jnp.concatenate(
        [
            jnp.broadcast_to(attended[None], (chips, count_local, heads)),
            hidden.reshape(count_local, chips, cores * block).transpose(1, 0, 2),
        ],
        axis=-1,
    )
    arrived = lax.all_to_all(pieces, PLANE, 0, 0, tiled=True).reshape(tokens // 2, -1)
    passed = shifted(arrived, "shard_2", 1)

    def project(rows):
        return lax.dot_general(
            out_weight, rows[:, :heads], (((0,), (1,)), ((), ())), preferred_element_type=F32
        ).astype(BF16)

    def my_columns(rows):
        return jnp.where(core == 0, rows[:, heads : heads + block], rows[:, heads + block :])

    part = jnp.concatenate([project(arrived), project(passed)], axis=1)
    hidden_t = jnp.concatenate([my_columns(arrived), my_columns(passed)], axis=0).T
    local = gate_weight.shape[0]
    place = jnp.stack([core, shard, group * local, (group == 0).astype(jnp.int32)]).astype(jnp.int32)
    ids = expert_ids.reshape(chips, cores, count_local, 2).transpose(3, 1, 0, 2).reshape(2, tokens)
    gain = jnp.broadcast_to(norm_gain[:, None], (width, 128))
    attn_out, (place, ids, gain, hidden_t) = sum_over_groups(part, (place, ids, gain, hidden_t))
    stream = (attn_out + hidden_t.astype(F32)).astype(BF16)
    own = lax.all_to_all(
        jnp.broadcast_to(stream[None], (chips, block, tokens)), PLANE, 0, 0, tiled=True
    )
    units = local * gate_weight.shape[2]
    partner = shifted(own, "shard_2", 1)
    send, keep = experts(
        place,
        own,
        partner,
        ids,
        gain,
        router.T,
        attn_out.astype(BF16),
        gate_weight.transpose(0, 2, 1).reshape(units, width),
        up_weight.transpose(0, 2, 1).reshape(units, width),
        down_weight.reshape(units, width),
    )
    pair = (keep.astype(F32) + shifted(send, "shard_2", 1).astype(F32)).astype(BF16)
    parts = lax.all_to_all(pair.reshape(chips, count_local, width), PLANE, 0, 0, tiled=True)
    reduced = parts.astype(F32).sum(axis=0).astype(BF16)
    return (hidden.astype(F32) + sum_over_groups(reduced)).astype(BF16)


def solution(mesh):
    split = Mesh(
        mesh.devices.reshape(mesh.shape["expert"], 4, 4, 2),
        ("expert", "shard_0", "shard_1", "shard_2"),
    )
    in_specs = (
        P(SHARD, None),
        P(SHARD, "expert", None),
        P(SHARD, None, "expert", None),
        P(SHARD, None, "expert", None),
        P("expert", SHARD),
        P(),
        P(),
        P(),
        P("expert", None, SHARD),
        P("expert", None, SHARD),
        P("expert", SHARD, None),
    )
    return jax.shard_map(
        on_device, mesh=split, in_specs=in_specs, out_specs=P(SHARD, None), check_vma=False
    )
```

```python
import math

import jax
import jax.numpy as jnp
from jax import lax
from jax.experimental import pallas as pl
from jax.experimental.pallas import tpu as pltpu
from jax.sharding import Mesh
from jax.sharding import PartitionSpec as P

SHARD = ("shard_0", "shard_1", "shard_2")
PLANE = ("shard_0", "shard_1")
F32 = jnp.float32
BF16 = jnp.bfloat16


def shifted(x, axis, by):
    size = lax.axis_size(axis)
    return lax.ppermute(x, axis, [(i, (i + by) % size) for i in range(size)])


def sum_over_groups(part, ready=()):
    others = tuple(shifted(part, "expert", by) for by in (1, 2, 3))
    (one, two, three), ready = lax.optimization_barrier((others, ready))
    total = (part.astype(F32) + two.astype(F32)) + (one.astype(F32) + three.astype(F32))
    return (total, ready) if ready else total


def bring_kernel(_, gate, up, down, held, sems):
    units = gate.shape[0]
    copies = [
        pltpu.make_async_copy(source, held.at[pl.ds(n * units, units)], sems.at[n])
        for n, source in enumerate((gate, up, down))
    ]
    for copy in copies:
        copy.start()
    for copy in copies:
        copy.wait()


def brought_in(after, *weights):
    size = sum(w.size for w in weights)
    rows, width = weights[0].shape
    return pl.pallas_call(
        bring_kernel,
        out_shape=pltpu.VMEM((3 * rows, width), BF16),
        in_specs=[pl.BlockSpec(memory_space=pl.ANY)] * 4,
        out_specs=pl.BlockSpec(memory_space=pltpu.VMEM),
        scratch_shapes=[pltpu.SemaphoreType.DMA((3,))],
        compiler_params=pltpu.CompilerParams(vmem_limit_bytes=36 * 1024 * 1024),
        cost_estimate=pl.CostEstimate(flops=80 * size, bytes_accessed=4 * size, transcendentals=0),
        name="bring",
    )(after, *weights)


def expert_kernel(place, ids, gain, router, attn, held, *refs):
    streams, (send, keep, mixed, hidden_t, act) = refs[:-5], refs[-5:]
    core, far, near, first_expert, adds = (place[n] for n in range(5))
    units, width = held.shape[0] // 3, held.shape[1]
    half_units = units // 2
    spread, block, tokens = streams[0].shape
    half = tokens // 2
    step = width // 4

    squares = jnp.zeros((8, tokens), F32)
    for n, part in enumerate(streams):
        by, is_partner = n // 2, n % 2
        here = (far - by) & (spread - 1)

        def norm_block(r, squares):
            x = part[r]
            if is_partner:
                x = jnp.concatenate([x[:, half:], x[:, :half]], axis=1)
            chip = here * spread + ((near - r) & (spread - 1))
            shard = 2 * chip + (1 - core if is_partner else core)
            rows = pl.ds(pl.multiple_of(shard * block, block), block)
            g = gain[rows, :]
            y = x.astype(F32)
            mixed[rows, :] = (y * jnp.concatenate([g, g], axis=1).astype(F32)).astype(BF16)
            return squares + (y * y).reshape(block // 8, 8, tokens).sum(axis=0)

        squares = lax.fori_loop(0, spread, norm_block, squares)
    scale = lax.rsqrt(squares.sum(axis=0, keepdims=True) / width + 1e-05)
    logits = jnp.dot(router[...], mixed[...], preferred_element_type=F32) * scale
    numbers = lax.broadcasted_iota(jnp.int32, logits.shape, 0)
    named = ids[...]
    named = jnp.where(
        core == 0, named, jnp.concatenate([named[:, half:], named[:, :half]], axis=1)
    )
    first, second = named[0:1, :], named[1:2, :]
    a = jnp.where(numbers == first, logits, 0.0).sum(axis=0, keepdims=True)
    b = jnp.where(numbers == second, logits, 0.0).sum(axis=0, keepdims=True)
    weight_first = 1.0 / (1.0 + jnp.exp(b - a))
    weight_second = 1.0 / (1.0 + jnp.exp(a - b))

    def expert_part(m, carry):
        for n in range(2):
            rows = pl.ds(pl.multiple_of((2 * n + m) * half_units, half_units), half_units)
            hidden_t[n] = jnp.dot(held[rows, :], mixed[...], preferred_element_type=F32)
        expert = first_expert + m
        routed = jnp.where(first == expert, weight_first, 0.0) + jnp.where(
            second == expert, weight_second, 0.0
        )
        gated = hidden_t[0] * scale
        upward = hidden_t[1] * scale
        value = gated / (1.0 + jnp.exp(-gated)) * upward * routed
        act[m] = value.T.astype(BF16)
        return carry

    lax.fori_loop(0, 2, expert_part, 0)

    def down_part(n, carry):
        columns = pl.ds(pl.multiple_of(n * step, step), step)
        total = jnp.dot(
            act[0], held[pl.ds(2 * units, half_units), columns], preferred_element_type=F32
        ) + jnp.dot(
            act[1], held[pl.ds(2 * units + half_units, half_units), columns], preferred_element_type=F32
        )
        keep[:, columns] = total[:half].astype(BF16)
        send[:, columns] = total[half:].astype(BF16)
        return carry

    lax.fori_loop(0, width // step, down_part, 0)
    rows = attn[...].astype(F32).T * adds.astype(F32)
    shard = 2 * (far * spread + near) + core
    columns = pl.ds(pl.multiple_of(shard * block, block), block)
    keep[:, columns] = (keep[:, columns].astype(F32) + rows[:half]).astype(BF16)
    send[:, columns] = (send[:, columns].astype(F32) + rows[half:]).astype(BF16)


def experts(place, ids, gain, router, attn, held, *streams):
    units, width = held.shape[0] // 3, held.shape[1]
    tokens = attn.shape[1]
    vmem = pl.BlockSpec(memory_space=pltpu.VMEM)
    half = jax.ShapeDtypeStruct((tokens // 2, width), BF16)
    return pl.pallas_call(
        expert_kernel,
        out_shape=(half, half),
        in_specs=[pl.BlockSpec(memory_space=pltpu.SMEM)] + [vmem] * (5 + len(streams)),
        out_specs=(vmem, vmem),
        scratch_shapes=[
            pltpu.VMEM((width, tokens), BF16),
            pltpu.VMEM((2, units // 2, tokens), F32),
            pltpu.VMEM((2, tokens, units // 2), BF16),
        ],
        compiler_params=pltpu.CompilerParams(vmem_limit_bytes=12 * 1024 * 1024),
        cost_estimate=pl.CostEstimate(
            flops=6 * tokens * units * width,
            bytes_accessed=6 * units * width,
            transcendentals=2 * units * tokens,
        ),
        name="experts",
    )(place, ids, gain, router, attn, held, *streams)


def on_device(
    hidden, queries, key_cache, value_cache, out_weight, norm_gain, router,
    expert_ids, gate_weight, up_weight, down_weight,
):
    count_local, heads_local, head_size = queries.shape
    kv_local = key_cache.shape[2]
    width = hidden.shape[1]
    block = out_weight.shape[1]
    chips, cores = lax.axis_size(PLANE), lax.axis_size("shard_2")
    tokens = chips * cores * count_local
    core = lax.axis_index("shard_2")
    group = lax.axis_index("expert")
    query_blocks = queries.reshape(count_local, kv_local, heads_local // kv_local, head_size)
    scores = jnp.einsum(
        "tkgd,tpkd->tkgp", query_blocks, key_cache, preferred_element_type=F32
    ) / math.sqrt(head_size)
    attn_weights = jax.nn.softmax(scores, axis=-1).astype(BF16)
    attended = jnp.einsum(
        "tkgp,tpkd->tkgd", attn_weights, value_cache, preferred_element_type=F32
    )
    heads = heads_local * head_size
    attended = attended.astype(BF16).reshape(count_local, heads)
    pieces = jnp.concatenate(
        [
            jnp.broadcast_to(attended[None], (chips, count_local, heads)),
            hidden.reshape(count_local, chips, cores * block).transpose(1, 0, 2),
        ],
        axis=-1,
    )
    arrived = lax.all_to_all(pieces, PLANE, 0, 0, tiled=True).reshape(tokens // 2, -1)
    passed = shifted(arrived, "shard_2", 1)

    def project(rows):
        return lax.dot_general(
            out_weight, rows[:, :heads], (((0,), (1,)), ((), ())), preferred_element_type=F32
        ).astype(BF16)

    def my_columns(rows):
        return jnp.where(core == 0, rows[:, heads : heads + block], rows[:, heads + block :])

    part = jnp.concatenate([project(arrived), project(passed)], axis=1)
    hidden_t = jnp.concatenate([my_columns(arrived), my_columns(passed)], axis=0).T
    local = gate_weight.shape[0]
    place = jnp.stack(
        [
            core,
            lax.axis_index("shard_0"),
            lax.axis_index("shard_1"),
            group * local,
            (group == 0).astype(jnp.int32),
        ]
    ).astype(jnp.int32)
    ids = expert_ids.reshape(chips, cores, count_local, 2).transpose(3, 1, 0, 2).reshape(2, tokens)
    gain = jnp.broadcast_to(norm_gain[:, None], (width, 128))
    attn_out, (place, ids, gain, hidden_t) = sum_over_groups(part, (place, ids, gain, hidden_t))
    stream = (attn_out + hidden_t.astype(F32)).astype(BF16)
    row = [stream] + [shifted(stream, "shard_1", by) for by in (1, 2, 3)]
    line = jnp.stack(row)
    plane = [line] + [shifted(line, "shard_0", by) for by in (1, 2, 3)]
    units = local * gate_weight.shape[2]
    held = brought_in(
        row[-1],
        gate_weight.transpose(0, 2, 1).reshape(units, width),
        up_weight.transpose(0, 2, 1).reshape(units, width),
        down_weight.reshape(units, width),
    )
    plane, held = lax.optimization_barrier((plane, held))
    streams = [x for part in plane for x in (part, shifted(part, "shard_2", 1))]
    send, keep = experts(
        place, ids, gain, router.T, attn_out.astype(BF16), held, *streams
    )
    pair = (keep.astype(F32) + shifted(send, "shard_2", 1).astype(F32)).astype(BF16)
    parts = lax.all_to_all(pair.reshape(chips, count_local, width), PLANE, 0, 0, tiled=True)
    reduced = parts.astype(F32).sum(axis=0).astype(BF16)
    return (hidden.astype(F32) + sum_over_groups(reduced)).astype(BF16)


def solution(mesh):
    split = Mesh(
        mesh.devices.reshape(mesh.shape["expert"], 4, 4, 2),
        ("expert", "shard_0", "shard_1", "shard_2"),
    )
    in_specs = (
        P(SHARD, None),
        P(SHARD, "expert", None),
        P(SHARD, None, "expert", None),
        P(SHARD, None, "expert", None),
        P("expert", SHARD),
        P(),
        P(),
        P(),
        P("expert", None, SHARD),
        P("expert", None, SHARD),
        P("expert", SHARD, None),
    )
    return jax.shard_map(
        on_device, mesh=split, in_specs=in_specs, out_specs=P(SHARD, None), check_vma=False
    )
```

```python
import math

import jax
import jax.numpy as jnp
from jax import lax
from jax.experimental import pallas as pl
from jax.experimental.pallas import tpu as pltpu
from jax.sharding import Mesh
from jax.sharding import PartitionSpec as P

SHARD = ("shard_0", "shard_1", "shard_2")
PLANE = ("shard_0", "shard_1")
F32 = jnp.float32
BF16 = jnp.bfloat16


def shifted(x, axis, by):
    size = lax.axis_size(axis)
    return lax.ppermute(x, axis, [(i, (i + by) % size) for i in range(size)])


def sum_over_groups(part, ready=()):
    others = tuple(shifted(part, "expert", by) for by in (1, 2, 3))
    (one, two, three), ready = lax.optimization_barrier((others, ready))
    total = (part.astype(F32) + two.astype(F32)) + (one.astype(F32) + three.astype(F32))
    return (total, ready) if ready else total


def attention_kernel(queries, hidden, key_hbm, value_hbm, pieces, keys, values, scores, found, sems):
    tokens, rows, size = keys.shape
    heads = queries.shape[0] // tokens
    kv_local = 2
    parts = sems.shape[1]
    count = tokens // parts

    def copy(n, part):
        source, target = ((key_hbm, keys), (value_hbm, values))[n]
        at = pl.ds(part * count, count)
        return pltpu.make_async_copy(source.at[at], target.at[at], sems.at[n, part])

    for n in range(2):
        for part in range(parts):
            copy(n, part).start()

    def score_part(part, carry):
        copy(0, part).wait()
        for m in range(count):
            t = part * count + m
            at = pl.ds(pl.multiple_of(t * heads, heads), heads)
            scores[at, :] = lax.dot_general(
                queries[at, :], keys[t], (((1,), (1,)), ((), ())), preferred_element_type=F32
            )
        return carry

    lax.fori_loop(0, parts, score_part, 0)
    chips, _, columns = pieces.shape
    block = columns - heads * size
    for chip in range(chips):
        pieces[chip, :, heads * size :] = hidden[:, chip * block : (chip + 1) * block]
    shape = scores.shape
    mine = (lax.broadcasted_iota(jnp.int32, shape, 0) % heads) // (heads // kv_local) == (
        lax.broadcasted_iota(jnp.int32, shape, 1) % kv_local
    )
    logits = jnp.where(mine, scores[...] * (1.0 / math.sqrt(size)), -3.0e38)
    powers = jnp.exp(logits - logits.max(axis=1, keepdims=True))
    scores[...] = powers / powers.sum(axis=1, keepdims=True)

    def wait_part(part, carry):
        copy(1, part).wait()
        return carry

    lax.fori_loop(0, parts, wait_part, 0)
    for t in range(tokens):
        at = pl.ds(t * heads, heads)
        found[at, :] = jnp.dot(
            scores[at, :].astype(BF16), values[t], preferred_element_type=F32
        )
    for h in range(heads):
        attended = found[pl.ds(h, tokens, stride=heads), :].astype(BF16)
        for chip in range(chips):
            pieces[chip, :, h * size : (h + 1) * size] = attended


def attention(queries, keys, values, hidden, chips):
    tokens, heads, size = queries.shape
    rows = keys.shape[1]
    width = heads * size + hidden.shape[1] // chips
    vmem = pl.BlockSpec(memory_space=pltpu.VMEM)
    hbm = pl.BlockSpec(memory_space=pl.ANY)
    return pl.pallas_call(
        attention_kernel,
        out_shape=jax.ShapeDtypeStruct((chips, tokens, width), BF16),
        in_specs=[vmem, vmem, hbm, hbm],
        out_specs=vmem,
        scratch_shapes=[
            pltpu.VMEM((tokens, rows, size), BF16),
            pltpu.VMEM((tokens, rows, size), BF16),
            pltpu.VMEM((tokens * heads, rows), F32),
            pltpu.VMEM((tokens * heads, size), F32),
            pltpu.SemaphoreType.DMA((2, 4)),
        ],
        compiler_params=pltpu.CompilerParams(vmem_limit_bytes=62 * 1024 * 1024),
        cost_estimate=pl.CostEstimate(
            flops=4 * tokens * heads * rows * size,
            bytes_accessed=4 * tokens * rows * size,
            transcendentals=tokens * heads * rows,
        ),
        name="attention",
    )(queries.reshape(tokens * heads, size), hidden, keys, values)


def bring_kernel(_, gains, gate, up, down, held, gain, sems):
    units = gate.shape[0]
    copies = [
        pltpu.make_async_copy(source, held.at[pl.ds(n * units, units)], sems.at[n])
        for n, source in enumerate((gate, up, down))
    ]
    for copy in copies:
        copy.start()
    lanes = gain.shape[1]
    for at in range(0, gain.shape[0], lanes):
        row = gains[:, at : at + lanes].astype(F32)
        gain[at : at + lanes, :] = jnp.broadcast_to(row, (lanes, lanes)).T.astype(BF16)
    for copy in copies:
        copy.wait()


def brought_in(after, gains, *weights):
    size = sum(w.size for w in weights)
    rows, width = weights[0].shape
    hbm = pl.BlockSpec(memory_space=pl.ANY)
    vmem = pl.BlockSpec(memory_space=pltpu.VMEM)
    return pl.pallas_call(
        bring_kernel,
        out_shape=(pltpu.VMEM((3 * rows, width), BF16), jax.ShapeDtypeStruct((width, 128), BF16)),
        in_specs=[hbm, vmem] + [hbm] * len(weights),
        out_specs=(vmem, vmem),
        scratch_shapes=[pltpu.SemaphoreType.DMA((3,))],
        compiler_params=pltpu.CompilerParams(vmem_limit_bytes=36 * 1024 * 1024),
        cost_estimate=pl.CostEstimate(flops=80 * size, bytes_accessed=4 * size, transcendentals=0),
        name="bring",
    )(after, gains, *weights)


def expert_kernel(
    place, ids, gain, router, attn, held, own, partner, send, keep, mixed, hidden_t, act
):
    core, shard, first_expert, adds = (place[n] for n in range(4))
    units, width = held.shape[0] // 3, held.shape[1]
    half_units = units // 2
    chips, block, tokens = own.shape
    half = tokens // 2

    def norm_block(j, squares):
        for mine, part in ((core, own), (1 - core, partner)):
            x = part[j]
            if part is partner:
                x = jnp.concatenate([x[:, half:], x[:, :half]], axis=1)
            rows = pl.ds(pl.multiple_of((2 * j + mine) * block, block), block)
            g = gain[rows, :]
            mixed[rows, :] = x * jnp.concatenate([g, g], axis=1)
            y = x.astype(F32)
            squares = squares + (y * y).reshape(block // 8, 8, tokens).sum(axis=0)
        return squares

    squares = lax.fori_loop(0, chips, norm_block, jnp.zeros((8, tokens), F32), unroll=4)
    scale = lax.rsqrt(squares.sum(axis=0, keepdims=True) / width + 1e-05)
    logits = jnp.dot(router[...], mixed[...], preferred_element_type=F32) * scale
    numbers = lax.broadcasted_iota(jnp.int32, logits.shape, 0)
    named = ids[...]
    named = jnp.where(
        core == 0, named, jnp.concatenate([named[:, half:], named[:, :half]], axis=1)
    )
    first, second = named[0:1, :], named[1:2, :]
    a = jnp.where(numbers == first, logits, 0.0).sum(axis=0, keepdims=True)
    b = jnp.where(numbers == second, logits, 0.0).sum(axis=0, keepdims=True)
    weight_first = 1.0 / (1.0 + jnp.exp(b - a))
    weight_second = 1.0 / (1.0 + jnp.exp(a - b))

    for m in range(2):
        for n in range(2):
            rows = pl.ds((2 * n + m) * half_units, half_units)
            hidden_t[m, n] = jnp.dot(held[rows, :], mixed[...], preferred_element_type=F32)
        expert = first_expert + m
        routed = jnp.where(first == expert, weight_first, 0.0) + jnp.where(
            second == expert, weight_second, 0.0
        )
        gated = hidden_t[m, 0] * scale
        upward = hidden_t[m, 1] * scale
        value = gated / (1.0 + jnp.exp(-gated)) * upward * routed
        act[m] = value.T.astype(BF16)

    step = width // 2

    def down_part(n, carry):
        columns = pl.ds(pl.multiple_of(n * step, step), step)
        total = jnp.dot(
            act[0], held[pl.ds(2 * units, half_units), columns], preferred_element_type=F32
        ) + jnp.dot(
            act[1],
            held[pl.ds(2 * units + half_units, half_units), columns],
            preferred_element_type=F32,
        )
        keep[:, columns] = total[:half].astype(BF16)
        send[:, columns] = total[half:].astype(BF16)
        return carry

    lax.fori_loop(0, width // step, down_part, 0)
    rows = attn[...].astype(F32).T * adds.astype(F32)
    columns = pl.ds(pl.multiple_of(shard * block, block), block)
    keep[:, columns] = (keep[:, columns].astype(F32) + rows[:half]).astype(BF16)
    send[:, columns] = (send[:, columns].astype(F32) + rows[half:]).astype(BF16)


def experts(place, ids, gain, router, attn, held, own, partner):
    units, width = held.shape[0] // 3, held.shape[1]
    tokens = attn.shape[1]
    vmem = pl.BlockSpec(memory_space=pltpu.VMEM)
    half = jax.ShapeDtypeStruct((tokens // 2, width), BF16)
    return pl.pallas_call(
        expert_kernel,
        out_shape=(half, half),
        in_specs=[pl.BlockSpec(memory_space=pltpu.SMEM)] + [vmem] * 7,
        out_specs=(vmem, vmem),
        scratch_shapes=[
            pltpu.VMEM((width, tokens), BF16),
            pltpu.VMEM((2, 2, units // 2, tokens), F32),
            pltpu.VMEM((2, tokens, units // 2), BF16),
        ],
        compiler_params=pltpu.CompilerParams(vmem_limit_bytes=12 * 1024 * 1024),
        cost_estimate=pl.CostEstimate(
            flops=6 * tokens * units * width,
            bytes_accessed=6 * units * width,
            transcendentals=2 * units * tokens,
        ),
        name="experts",
    )(place, ids, gain, router, attn, held, own, partner)


def on_device(
    hidden, queries, key_cache, value_cache, out_weight, norm_gain, router,
    expert_ids, gate_weight, up_weight, down_weight,
):
    count_local, heads_local, head_size = queries.shape
    kv_local = key_cache.shape[2]
    width = hidden.shape[1]
    block = out_weight.shape[1]
    chips, cores = lax.axis_size(PLANE), lax.axis_size("shard_2")
    tokens = chips * cores * count_local
    core = lax.axis_index("shard_2")
    group = lax.axis_index("expert")
    heads = heads_local * head_size
    rows = key_cache.shape[1] * kv_local
    pieces = attention(
        queries,
        key_cache.reshape(count_local, rows, head_size),
        value_cache.reshape(count_local, rows, head_size),
        hidden,
        chips,
    )
    local = gate_weight.shape[0]
    units = local * gate_weight.shape[2]
    place = jnp.stack(
        [
            core,
            lax.axis_index(PLANE) * cores + core,
            group * local,
            (group == 0).astype(jnp.int32),
        ]
    ).astype(jnp.int32)
    ids = expert_ids.reshape(chips, cores, count_local, 2).transpose(3, 1, 0, 2).reshape(2, tokens)
    arrived = lax.all_to_all(pieces, PLANE, 0, 0, tiled=True).reshape(tokens // 2, -1)
    arrived, place, ids = lax.optimization_barrier((arrived, place, ids))
    passed = shifted(arrived, "shard_2", 1)

    def project(rows):
        return lax.dot_general(
            out_weight, rows[:, :heads], (((0,), (1,)), ((), ())), preferred_element_type=F32
        ).astype(BF16)

    def my_columns(rows):
        return jnp.where(core == 0, rows[:, heads : heads + block], rows[:, heads + block :])

    part = jnp.concatenate([project(arrived), project(passed)], axis=1)
    hidden_t = jnp.concatenate([my_columns(arrived), my_columns(passed)], axis=0).T
    held, gain = brought_in(
        part,
        norm_gain[None, :],
        gate_weight.transpose(0, 2, 1).reshape(units, width),
        up_weight.transpose(0, 2, 1).reshape(units, width),
        down_weight.reshape(units, width),
    )
    attn_out, (hidden_t, held, gain) = sum_over_groups(part, (hidden_t, held, gain))
    stream = (attn_out + hidden_t.astype(F32)).astype(BF16)
    own = lax.all_to_all(
        jnp.broadcast_to(stream[None], (chips, block, tokens)), PLANE, 0, 0, tiled=True
    )
    partner = shifted(own, "shard_2", 1)
    send, keep = experts(
        place, ids, gain, router.T, attn_out.astype(BF16), held, own, partner
    )
    pair = (keep.astype(F32) + shifted(send, "shard_2", 1).astype(F32)).astype(BF16)
    parts = lax.all_to_all(pair.reshape(chips, count_local, width), PLANE, 0, 0, tiled=True)
    reduced = parts.astype(F32).sum(axis=0).astype(BF16)
    return (hidden.astype(F32) + sum_over_groups(reduced)).astype(BF16)


def solution(mesh):
    split = Mesh(
        mesh.devices.reshape(mesh.shape["expert"], 4, 4, 2),
        ("expert", "shard_0", "shard_1", "shard_2"),
    )
    in_specs = (
        P(SHARD, None),
        P(SHARD, "expert", None),
        P(SHARD, None, "expert", None),
        P(SHARD, None, "expert", None),
        P("expert", SHARD),
        P(),
        P(),
        P(),
        P("expert", None, SHARD),
        P("expert", None, SHARD),
        P("expert", SHARD, None),
    )
    return jax.shard_map(
        on_device, mesh=split, in_specs=in_specs, out_specs=P(SHARD, None), check_vma=False
    )
```

```python
import math

import jax
import jax.numpy as jnp
from jax import lax
from jax.experimental import pallas as pl
from jax.experimental.pallas import tpu as pltpu
from jax.sharding import Mesh
from jax.sharding import PartitionSpec as P

SHARD = ("shard_0", "shard_1", "shard_2")
PLANE = ("shard_0", "shard_1")
F32 = jnp.float32
BF16 = jnp.bfloat16
BRING_GRANT = 40 * 1024 * 1024
EXPERT_GRANT = 36 * 1024 * 1024


def shifted(x, axis, by):
    size = lax.axis_size(axis)
    return lax.ppermute(x, axis, [(i, (i + by) % size) for i in range(size)])


def sum_over_groups(part, ready=()):
    others = tuple(shifted(part, "expert", by) for by in (1, 2, 3))
    (one, two, three), ready = lax.optimization_barrier((others, ready))
    total = (part.astype(F32) + two.astype(F32)) + (one.astype(F32) + three.astype(F32))
    return (total, ready) if ready else total


def attention_kernel(queries, hidden, key_hbm, value_hbm, pieces, keys, values, scores, found, sems):
    tokens, rows, size = keys.shape
    heads = queries.shape[0] // tokens
    kv_local = 2
    parts = sems.shape[1]
    count = tokens // parts

    def copy(n, part):
        source, target = ((key_hbm, keys), (value_hbm, values))[n]
        at = pl.ds(part * count, count)
        return pltpu.make_async_copy(source.at[at], target.at[at], sems.at[n, part])

    for n in range(2):
        for part in range(parts):
            copy(n, part).start()

    def score_part(part, carry):
        copy(0, part).wait()
        for m in range(count):
            t = part * count + m
            at = pl.ds(pl.multiple_of(t * heads, heads), heads)
            scores[at, :] = lax.dot_general(
                queries[at, :], keys[t], (((1,), (1,)), ((), ())), preferred_element_type=F32
            )
        return carry

    lax.fori_loop(0, parts, score_part, 0)
    chips, _, columns = pieces.shape
    block = columns - heads * size
    for chip in range(chips):
        pieces[chip, :, heads * size :] = hidden[:, chip * block : (chip + 1) * block]
    shape = scores.shape
    mine = (lax.broadcasted_iota(jnp.int32, shape, 0) % heads) // (heads // kv_local) == (
        lax.broadcasted_iota(jnp.int32, shape, 1) % kv_local
    )
    logits = jnp.where(mine, scores[...] * (1.0 / math.sqrt(size)), -3.0e38)
    powers = jnp.exp(logits - logits.max(axis=1, keepdims=True))
    scores[...] = powers / powers.sum(axis=1, keepdims=True)

    def wait_part(part, carry):
        copy(1, part).wait()
        return carry

    lax.fori_loop(0, parts, wait_part, 0)
    for t in range(tokens):
        at = pl.ds(t * heads, heads)
        found[at, :] = jnp.dot(
            scores[at, :].astype(BF16), values[t], preferred_element_type=F32
        )
    for h in range(heads):
        attended = found[pl.ds(h, tokens, stride=heads), :].astype(BF16)
        for chip in range(chips):
            pieces[chip, :, h * size : (h + 1) * size] = attended


def attention(queries, keys, values, hidden, chips):
    tokens, heads, size = queries.shape
    rows = keys.shape[1]
    width = heads * size + hidden.shape[1] // chips
    vmem = pl.BlockSpec(memory_space=pltpu.VMEM)
    hbm = pl.BlockSpec(memory_space=pl.ANY)
    return pl.pallas_call(
        attention_kernel,
        out_shape=jax.ShapeDtypeStruct((chips, tokens, width), BF16),
        in_specs=[vmem, vmem, hbm, hbm],
        out_specs=vmem,
        scratch_shapes=[
            pltpu.VMEM((tokens, rows, size), BF16),
            pltpu.VMEM((tokens, rows, size), BF16),
            pltpu.VMEM((tokens * heads, rows), F32),
            pltpu.VMEM((tokens * heads, size), F32),
            pltpu.SemaphoreType.DMA((2, 4)),
        ],
        compiler_params=pltpu.CompilerParams(vmem_limit_bytes=62 * 1024 * 1024),
        cost_estimate=pl.CostEstimate(
            flops=4 * tokens * heads * rows * size,
            bytes_accessed=4 * tokens * rows * size,
            transcendentals=tokens * heads * rows,
        ),
        name="attention",
    )(queries.reshape(tokens * heads, size), hidden, keys, values)


def spread_kernel(_, gains, gain):
    lanes = gain.shape[1]
    for at in range(0, gain.shape[0], lanes):
        row = gains[:, at : at + lanes].astype(F32)
        gain[at : at + lanes, :] = jnp.broadcast_to(row, (lanes, lanes)).T.astype(BF16)


def spread(after, gains):
    size = gains.shape[1]
    vmem = pl.BlockSpec(memory_space=pltpu.VMEM)
    return pl.pallas_call(
        spread_kernel,
        out_shape=jax.ShapeDtypeStruct((size, 128), BF16),
        in_specs=[pl.BlockSpec(memory_space=pl.ANY), vmem],
        out_specs=vmem,
        compiler_params=pltpu.CompilerParams(vmem_limit_bytes=4 * 1024 * 1024),
        cost_estimate=pl.CostEstimate(
            flops=20000 * size, bytes_accessed=256 * size, transcendentals=0
        ),
        name="spread",
    )(after, gains)


def bring_kernel(_, source, target, sem):
    copy = pltpu.make_async_copy(source, target, sem)
    copy.start()
    copy.wait()


def brought_in(after, weights):
    hbm = pl.BlockSpec(memory_space=pl.ANY)
    return pl.pallas_call(
        bring_kernel,
        out_shape=pltpu.VMEM(weights.shape, weights.dtype),
        in_specs=[hbm, hbm],
        out_specs=pl.BlockSpec(memory_space=pltpu.VMEM),
        scratch_shapes=[pltpu.SemaphoreType.DMA],
        compiler_params=pltpu.CompilerParams(vmem_limit_bytes=BRING_GRANT),
        cost_estimate=pl.CostEstimate(
            flops=80 * weights.size, bytes_accessed=4 * weights.size, transcendentals=0
        ),
        name="bring",
    )(after, weights)


def expert_kernel(
    place, ids, gain, router, attn, gate, own, partner, up_hbm, down_hbm,
    send, keep, mixed, hidden_t, act, up, down, sems,
):
    core, shard, first_expert, adds = (place[n] for n in range(4))
    units, width = gate.shape
    half_units = units // 2
    chips, block, tokens = own.shape
    half = tokens // 2
    step = width // 2

    def up_copy(m):
        rows = pl.ds(pl.multiple_of(m * half_units, half_units), half_units)
        return pltpu.make_async_copy(up_hbm.at[rows], up.at[rows], sems.at[m])

    def down_copy(n):
        columns = pl.ds(pl.multiple_of(n * step, step), step)
        return pltpu.make_async_copy(
            down_hbm.at[:, columns], down.at[:, columns], sems.at[2 + n]
        )

    for m in range(2):
        up_copy(m).start()
    for n in range(2):
        down_copy(n).start()

    def norm_block(j, squares):
        for mine, part in ((core, own), (1 - core, partner)):
            x = part[j]
            if part is partner:
                x = jnp.concatenate([x[:, half:], x[:, :half]], axis=1)
            rows = pl.ds(pl.multiple_of((2 * j + mine) * block, block), block)
            g = gain[rows, :]
            mixed[rows, :] = x * jnp.concatenate([g, g], axis=1)
            y = x.astype(F32)
            squares = squares + (y * y).reshape(block // 8, 8, tokens).sum(axis=0)
        return squares

    squares = lax.fori_loop(0, chips, norm_block, jnp.zeros((8, tokens), F32), unroll=4)
    scale = lax.rsqrt(squares.sum(axis=0, keepdims=True) / width + 1e-05)
    logits = jnp.dot(router[...], mixed[...], preferred_element_type=F32) * scale
    numbers = lax.broadcasted_iota(jnp.int32, logits.shape, 0)
    named = ids[...]
    named = jnp.where(
        core == 0, named, jnp.concatenate([named[:, half:], named[:, :half]], axis=1)
    )
    first, second = named[0:1, :], named[1:2, :]
    a = jnp.where(numbers == first, logits, 0.0).sum(axis=0, keepdims=True)
    b = jnp.where(numbers == second, logits, 0.0).sum(axis=0, keepdims=True)
    weight_first = 1.0 / (1.0 + jnp.exp(b - a))
    weight_second = 1.0 / (1.0 + jnp.exp(a - b))

    for m in range(2):
        rows = pl.ds(m * half_units, half_units)
        hidden_t[0, m] = jnp.dot(gate[rows, :], mixed[...], preferred_element_type=F32)

    def up_part(m, carry):
        up_copy(m).wait()
        rows = pl.ds(pl.multiple_of(m * half_units, half_units), half_units)
        hidden_t[1, m] = jnp.dot(up[rows, :], mixed[...], preferred_element_type=F32)
        return carry

    lax.fori_loop(0, 2, up_part, 0)
    for m in range(2):
        expert = first_expert + m
        routed = jnp.where(first == expert, weight_first, 0.0) + jnp.where(
            second == expert, weight_second, 0.0
        )
        gated = hidden_t[0, m] * scale
        upward = hidden_t[1, m] * scale
        value = gated / (1.0 + jnp.exp(-gated)) * upward * routed
        act[m] = value.T.astype(BF16)

    def down_part(n, carry):
        down_copy(n).wait()
        columns = pl.ds(pl.multiple_of(n * step, step), step)
        total = jnp.dot(
            act[0], down[pl.ds(0, half_units), columns], preferred_element_type=F32
        ) + jnp.dot(
            act[1], down[pl.ds(half_units, half_units), columns], preferred_element_type=F32
        )
        keep[:, columns] = total[:half].astype(BF16)
        send[:, columns] = total[half:].astype(BF16)
        return carry

    lax.fori_loop(0, 2, down_part, 0)
    rows = attn[...].astype(F32).T * adds.astype(F32)
    columns = pl.ds(pl.multiple_of(shard * block, block), block)
    keep[:, columns] = (keep[:, columns].astype(F32) + rows[:half]).astype(BF16)
    send[:, columns] = (send[:, columns].astype(F32) + rows[half:]).astype(BF16)


def experts(place, ids, gain, router, attn, gate, own, partner, up, down):
    units, width = gate.shape
    tokens = attn.shape[1]
    vmem = pl.BlockSpec(memory_space=pltpu.VMEM)
    hbm = pl.BlockSpec(memory_space=pl.ANY)
    half = jax.ShapeDtypeStruct((tokens // 2, width), BF16)
    return pl.pallas_call(
        expert_kernel,
        out_shape=(half, half),
        in_specs=[pl.BlockSpec(memory_space=pltpu.SMEM)] + [vmem] * 7 + [hbm] * 2,
        out_specs=(vmem, vmem),
        scratch_shapes=[
            pltpu.VMEM((width, tokens), BF16),
            pltpu.VMEM((2, 2, units // 2, tokens), F32),
            pltpu.VMEM((2, tokens, units // 2), BF16),
            pltpu.VMEM((units, width), BF16),
            pltpu.VMEM((units, width), BF16),
            pltpu.SemaphoreType.DMA((4,)),
        ],
        compiler_params=pltpu.CompilerParams(vmem_limit_bytes=EXPERT_GRANT),
        cost_estimate=pl.CostEstimate(
            flops=6 * tokens * units * width,
            bytes_accessed=6 * units * width,
            transcendentals=2 * units * tokens,
        ),
        name="experts",
    )(place, ids, gain, router, attn, gate, own, partner, up, down)


def on_device(
    hidden, queries, key_cache, value_cache, out_weight, norm_gain, router,
    expert_ids, gate_weight, up_weight, down_weight,
):
    count_local, heads_local, head_size = queries.shape
    kv_local = key_cache.shape[2]
    width = hidden.shape[1]
    block = out_weight.shape[1]
    chips, cores = lax.axis_size(PLANE), lax.axis_size("shard_2")
    tokens = chips * cores * count_local
    core = lax.axis_index("shard_2")
    group = lax.axis_index("expert")
    heads = heads_local * head_size
    rows = key_cache.shape[1] * kv_local
    pieces = attention(
        queries,
        key_cache.reshape(count_local, rows, head_size),
        value_cache.reshape(count_local, rows, head_size),
        hidden,
        chips,
    )
    local = gate_weight.shape[0]
    units = local * gate_weight.shape[2]
    place = jnp.stack(
        [
            core,
            lax.axis_index(PLANE) * cores + core,
            group * local,
            (group == 0).astype(jnp.int32),
        ]
    ).astype(jnp.int32)
    ids = expert_ids.reshape(chips, cores, count_local, 2).transpose(3, 1, 0, 2).reshape(2, tokens)
    arrived = lax.all_to_all(pieces, PLANE, 0, 0, tiled=True).reshape(tokens // 2, -1)
    arrived, place, ids = lax.optimization_barrier((arrived, place, ids))
    passed = shifted(arrived, "shard_2", 1)

    def project(rows):
        return lax.dot_general(
            out_weight, rows[:, :heads], (((0,), (1,)), ((), ())), preferred_element_type=F32
        ).astype(BF16)

    def my_columns(rows):
        return jnp.where(core == 0, rows[:, heads : heads + block], rows[:, heads + block :])

    part = jnp.concatenate([project(arrived), project(passed)], axis=1)
    hidden_t = jnp.concatenate([my_columns(arrived), my_columns(passed)], axis=0).T
    attn_out, (hidden_t,) = sum_over_groups(part, (hidden_t,))
    stream = (attn_out + hidden_t.astype(F32)).astype(BF16)
    own = lax.all_to_all(
        jnp.broadcast_to(stream[None], (chips, block, tokens)), PLANE, 0, 0, tiled=True
    )
    gain = spread(stream, norm_gain[None, :])
    own, gain = lax.optimization_barrier((own, gain))
    partner = shifted(own, "shard_2", 1)
    gate = brought_in(own, gate_weight.transpose(0, 2, 1).reshape(units, width))
    partner, gate = lax.optimization_barrier((partner, gate))
    send, keep = experts(
        place,
        ids,
        gain,
        router.T,
        attn_out.astype(BF16),
        gate,
        own,
        partner,
        up_weight.transpose(0, 2, 1).reshape(units, width),
        down_weight.reshape(units, width),
    )
    pair = (keep.astype(F32) + shifted(send, "shard_2", 1).astype(F32)).astype(BF16)
    parts = lax.all_to_all(pair.reshape(chips, count_local, width), PLANE, 0, 0, tiled=True)
    residual, _ = lax.optimization_barrier((hidden, pair))
    parts, residual = lax.optimization_barrier((parts, residual.astype(F32)))
    reduced = parts.astype(F32).sum(axis=0).astype(BF16)
    return (residual + sum_over_groups(reduced)).astype(BF16)


def solution(mesh):
    split = Mesh(
        mesh.devices.reshape(mesh.shape["expert"], 4, 4, 2),
        ("expert", "shard_0", "shard_1", "shard_2"),
    )
    in_specs = (
        P(SHARD, None),
        P(SHARD, "expert", None),
        P(SHARD, None, "expert", None),
        P(SHARD, None, "expert", None),
        P("expert", SHARD),
        P(),
        P(),
        P(),
        P("expert", None, SHARD),
        P("expert", None, SHARD),
        P("expert", SHARD, None),
    )
    return jax.shard_map(
        on_device, mesh=split, in_specs=in_specs, out_specs=P(SHARD, None), check_vma=False
    )
```

```python
import math

import jax
import jax.numpy as jnp
from jax import lax
from jax.experimental import pallas as pl
from jax.experimental.pallas import tpu as pltpu
from jax.sharding import Mesh
from jax.sharding import PartitionSpec as P

SHARD = ("shard_0", "shard_1", "shard_2")
PLANE = ("shard_0", "shard_1")
F32 = jnp.float32
BF16 = jnp.bfloat16
BRING_GRANT = 40 * 1024 * 1024
EXPERT_GRANT = 36 * 1024 * 1024


def shifted(x, axis, by):
    size = lax.axis_size(axis)
    return lax.ppermute(x, axis, [(i, (i + by) % size) for i in range(size)])


def sum_over_groups(part, ready=()):
    others = tuple(shifted(part, "expert", by) for by in (1, 2, 3))
    (one, two, three), ready = lax.optimization_barrier((others, ready))
    total = (part.astype(F32) + two.astype(F32)) + (one.astype(F32) + three.astype(F32))
    return (total, ready) if ready else total


def attention_kernel(queries, hidden, key_hbm, value_hbm, pieces, keys, values, scores, found, sems):
    tokens, rows, size = keys.shape
    heads = queries.shape[0] // tokens
    kv_local = 2
    parts = sems.shape[1]
    count = tokens // parts

    def copy(n, part):
        source, target = ((key_hbm, keys), (value_hbm, values))[n]
        at = pl.ds(part * count, count)
        return pltpu.make_async_copy(source.at[at], target.at[at], sems.at[n, part])

    for n in range(2):
        for part in range(parts):
            copy(n, part).start()

    def score_part(part, carry):
        copy(0, part).wait()
        for m in range(count):
            t = part * count + m
            at = pl.ds(pl.multiple_of(t * heads, heads), heads)
            scores[at, :] = lax.dot_general(
                queries[at, :], keys[t], (((1,), (1,)), ((), ())), preferred_element_type=F32
            )
        return carry

    lax.fori_loop(0, parts, score_part, 0)
    chips, _, columns = pieces.shape
    block = columns - heads * size
    for chip in range(chips):
        pieces[chip, :, heads * size :] = hidden[:, chip * block : (chip + 1) * block]
    shape = scores.shape
    mine = (lax.broadcasted_iota(jnp.int32, shape, 0) % heads) // (heads // kv_local) == (
        lax.broadcasted_iota(jnp.int32, shape, 1) % kv_local
    )
    logits = jnp.where(mine, scores[...] * (1.0 / math.sqrt(size)), -3.0e38)
    powers = jnp.exp(logits - logits.max(axis=1, keepdims=True))
    scores[...] = powers / powers.sum(axis=1, keepdims=True)

    def wait_part(part, carry):
        copy(1, part).wait()
        return carry

    lax.fori_loop(0, parts, wait_part, 0)
    for t in range(tokens):
        at = pl.ds(t * heads, heads)
        found[at, :] = jnp.dot(
            scores[at, :].astype(BF16), values[t], preferred_element_type=F32
        )
    for h in range(heads):
        attended = found[pl.ds(h, tokens, stride=heads), :].astype(BF16)
        for chip in range(chips):
            pieces[chip, :, h * size : (h + 1) * size] = attended


def attention(queries, keys, values, hidden, chips):
    tokens, heads, size = queries.shape
    rows = keys.shape[1]
    width = heads * size + hidden.shape[1] // chips
    vmem = pl.BlockSpec(memory_space=pltpu.VMEM)
    hbm = pl.BlockSpec(memory_space=pl.ANY)
    return pl.pallas_call(
        attention_kernel,
        out_shape=jax.ShapeDtypeStruct((chips, tokens, width), BF16),
        in_specs=[vmem, vmem, hbm, hbm],
        out_specs=vmem,
        scratch_shapes=[
            pltpu.VMEM((tokens, rows, size), BF16),
            pltpu.VMEM((tokens, rows, size), BF16),
            pltpu.VMEM((tokens * heads, rows), F32),
            pltpu.VMEM((tokens * heads, size), F32),
            pltpu.SemaphoreType.DMA((2, 4)),
        ],
        compiler_params=pltpu.CompilerParams(vmem_limit_bytes=62 * 1024 * 1024),
        cost_estimate=pl.CostEstimate(
            flops=4 * tokens * heads * rows * size,
            bytes_accessed=4 * tokens * rows * size,
            transcendentals=tokens * heads * rows,
        ),
        name="attention",
    )(queries.reshape(tokens * heads, size), hidden, keys, values)


def spread_kernel(_, gains, gain):
    lanes = gain.shape[1]
    for at in range(0, gain.shape[0], lanes):
        row = gains[:, at : at + lanes].astype(F32)
        gain[at : at + lanes, :] = jnp.broadcast_to(row, (lanes, lanes)).T.astype(BF16)


def spread(after, gains):
    size = gains.shape[1]
    vmem = pl.BlockSpec(memory_space=pltpu.VMEM)
    return pl.pallas_call(
        spread_kernel,
        out_shape=jax.ShapeDtypeStruct((size, 128), BF16),
        in_specs=[pl.BlockSpec(memory_space=pl.ANY), vmem],
        out_specs=vmem,
        compiler_params=pltpu.CompilerParams(vmem_limit_bytes=4 * 1024 * 1024),
        cost_estimate=pl.CostEstimate(
            flops=20000 * size, bytes_accessed=256 * size, transcendentals=0
        ),
        name="spread",
    )(after, gains)


def bring_kernel(_, source, target, sem):
    copy = pltpu.make_async_copy(source, target, sem)
    copy.start()
    copy.wait()


def brought_in(after, weights):
    hbm = pl.BlockSpec(memory_space=pl.ANY)
    return pl.pallas_call(
        bring_kernel,
        out_shape=pltpu.VMEM(weights.shape, weights.dtype),
        in_specs=[hbm, hbm],
        out_specs=pl.BlockSpec(memory_space=pltpu.VMEM),
        scratch_shapes=[pltpu.SemaphoreType.DMA],
        compiler_params=pltpu.CompilerParams(vmem_limit_bytes=BRING_GRANT),
        cost_estimate=pl.CostEstimate(
            flops=80 * weights.size, bytes_accessed=4 * weights.size, transcendentals=0
        ),
        name="bring",
    )(after, weights)


def expert_kernel(
    place, ids, gain, router, attn, gate, own, partner, up_hbm, down_hbm,
    send, keep, mixed, hidden_t, act, up, down, sems,
):
    core, shard, first_expert, adds = (place[n] for n in range(4))
    units, width = gate.shape
    half_units = units // 2
    chips, block, tokens = own.shape
    half = tokens // 2
    step = width // 2

    def up_copy(m):
        rows = pl.ds(pl.multiple_of(m * half_units, half_units), half_units)
        return pltpu.make_async_copy(up_hbm.at[rows], up.at[rows], sems.at[m])

    def down_copy(n):
        columns = pl.ds(pl.multiple_of(n * step, step), step)
        return pltpu.make_async_copy(
            down_hbm.at[:, columns], down.at[:, columns], sems.at[2 + n]
        )

    for m in range(2):
        up_copy(m).start()
    for n in range(2):
        down_copy(n).start()

    def norm_block(j, squares):
        for mine, part in ((core, own), (1 - core, partner)):
            x = part[j]
            if part is partner:
                x = jnp.concatenate([x[:, half:], x[:, :half]], axis=1)
            rows = pl.ds(pl.multiple_of((2 * j + mine) * block, block), block)
            g = gain[rows, :]
            mixed[rows, :] = x * jnp.concatenate([g, g], axis=1)
            y = x.astype(F32)
            squares = squares + (y * y).reshape(block // 8, 8, tokens).sum(axis=0)
        return squares

    squares = lax.fori_loop(0, chips, norm_block, jnp.zeros((8, tokens), F32), unroll=4)
    scale = lax.rsqrt(squares.sum(axis=0, keepdims=True) / width + 1e-05)
    logits = jnp.dot(router[...], mixed[...], preferred_element_type=F32) * scale
    numbers = lax.broadcasted_iota(jnp.int32, logits.shape, 0)
    named = ids[...]
    named = jnp.where(
        core == 0, named, jnp.concatenate([named[:, half:], named[:, :half]], axis=1)
    )
    first, second = named[0:1, :], named[1:2, :]
    a = jnp.where(numbers == first, logits, 0.0).sum(axis=0, keepdims=True)
    b = jnp.where(numbers == second, logits, 0.0).sum(axis=0, keepdims=True)
    weight_first = 1.0 / (1.0 + jnp.exp(b - a))
    weight_second = 1.0 / (1.0 + jnp.exp(a - b))

    for m in range(2):
        rows = pl.ds(m * half_units, half_units)
        hidden_t[0, m] = jnp.dot(gate[rows, :], mixed[...], preferred_element_type=F32)

    def up_part(m, carry):
        up_copy(m).wait()
        rows = pl.ds(pl.multiple_of(m * half_units, half_units), half_units)
        hidden_t[1, m] = jnp.dot(up[rows, :], mixed[...], preferred_element_type=F32)
        return carry

    lax.fori_loop(0, 2, up_part, 0)
    for m in range(2):
        expert = first_expert + m
        routed = jnp.where(first == expert, weight_first, 0.0) + jnp.where(
            second == expert, weight_second, 0.0
        )
        gated = hidden_t[0, m] * scale
        upward = hidden_t[1, m] * scale
        value = gated / (1.0 + jnp.exp(-gated)) * upward * routed
        act[m] = value.T.astype(BF16)

    def down_part(n, carry):
        down_copy(n).wait()
        columns = pl.ds(pl.multiple_of(n * step, step), step)
        total = jnp.dot(
            act[0], down[pl.ds(0, half_units), columns], preferred_element_type=F32
        ) + jnp.dot(
            act[1], down[pl.ds(half_units, half_units), columns], preferred_element_type=F32
        )
        keep[:, columns] = total[:half].astype(BF16)
        send[:, columns] = total[half:].astype(BF16)
        return carry

    lax.fori_loop(0, 2, down_part, 0)
    rows = attn[...].astype(F32).T * adds.astype(F32)
    columns = pl.ds(pl.multiple_of(shard * block, block), block)
    keep[:, columns] = (keep[:, columns].astype(F32) + rows[:half]).astype(BF16)
    send[:, columns] = (send[:, columns].astype(F32) + rows[half:]).astype(BF16)


def experts(place, ids, gain, router, attn, gate, own, partner, up, down):
    units, width = gate.shape
    tokens = attn.shape[1]
    vmem = pl.BlockSpec(memory_space=pltpu.VMEM)
    hbm = pl.BlockSpec(memory_space=pl.ANY)
    half = jax.ShapeDtypeStruct((tokens // 2, width), BF16)
    return pl.pallas_call(
        expert_kernel,
        out_shape=(half, half),
        in_specs=[pl.BlockSpec(memory_space=pltpu.SMEM)] + [vmem] * 7 + [hbm] * 2,
        out_specs=(vmem, vmem),
        scratch_shapes=[
            pltpu.VMEM((width, tokens), BF16),
            pltpu.VMEM((2, 2, units // 2, tokens), F32),
            pltpu.VMEM((2, tokens, units // 2), BF16),
            pltpu.VMEM((units, width), BF16),
            pltpu.VMEM((units, width), BF16),
            pltpu.SemaphoreType.DMA((4,)),
        ],
        compiler_params=pltpu.CompilerParams(vmem_limit_bytes=EXPERT_GRANT),
        cost_estimate=pl.CostEstimate(
            flops=6 * tokens * units * width,
            bytes_accessed=6 * units * width,
            transcendentals=2 * units * tokens,
        ),
        name="experts",
    )(place, ids, gain, router, attn, gate, own, partner, up, down)


def on_device(
    hidden, queries, key_cache, value_cache, out_weight, norm_gain, router,
    expert_ids, gate_weight, up_weight, down_weight,
):
    count_local, heads_local, head_size = queries.shape
    kv_local = key_cache.shape[2]
    width = hidden.shape[1]
    block = out_weight.shape[1]
    chips, cores = lax.axis_size(PLANE), lax.axis_size("shard_2")
    tokens = chips * cores * count_local
    core = lax.axis_index("shard_2")
    group = lax.axis_index("expert")
    heads = heads_local * head_size
    rows = key_cache.shape[1] * kv_local
    pieces = attention(
        queries,
        key_cache.reshape(count_local, rows, head_size),
        value_cache.reshape(count_local, rows, head_size),
        hidden,
        chips,
    )
    local = gate_weight.shape[0]
    units = local * gate_weight.shape[2]
    place = jnp.stack(
        [
            core,
            lax.axis_index(PLANE) * cores + core,
            group * local,
            (group == 0).astype(jnp.int32),
        ]
    ).astype(jnp.int32)
    ids = expert_ids.reshape(chips, cores, count_local, 2).transpose(3, 1, 0, 2).reshape(2, tokens)
    arrived = lax.all_to_all(pieces, PLANE, 0, 0, tiled=True).reshape(tokens // 2, -1)
    arrived, place, ids = lax.optimization_barrier((arrived, place, ids))
    passed = shifted(arrived, "shard_2", 1)

    def project(rows):
        return lax.dot_general(
            out_weight, rows[:, :heads], (((0,), (1,)), ((), ())), preferred_element_type=F32
        ).astype(BF16)

    def my_columns(rows):
        return jnp.where(core == 0, rows[:, heads : heads + block], rows[:, heads + block :])

    part = jnp.concatenate([project(arrived), project(passed)], axis=1)
    hidden_t = jnp.concatenate([my_columns(arrived), my_columns(passed)], axis=0).T
    gain = spread(part, norm_gain[None, :])
    attn_out, (hidden_t, gain) = sum_over_groups(part, (hidden_t, gain))
    stream = (attn_out + hidden_t.astype(F32)).astype(BF16)
    own = lax.all_to_all(
        jnp.broadcast_to(stream[None], (chips, block, tokens)), PLANE, 0, 0, tiled=True
    )
    partner = shifted(own, "shard_2", 1)
    gate = brought_in(own, gate_weight.transpose(0, 2, 1).reshape(units, width))
    partner, gate = lax.optimization_barrier((partner, gate))
    send, keep = experts(
        place,
        ids,
        gain,
        router.T,
        attn_out.astype(BF16),
        gate,
        own,
        partner,
        up_weight.transpose(0, 2, 1).reshape(units, width),
        down_weight.reshape(units, width),
    )
    pair = (keep.astype(F32) + shifted(send, "shard_2", 1).astype(F32)).astype(BF16)
    parts = lax.all_to_all(pair.reshape(chips, count_local, width), PLANE, 0, 0, tiled=True)
    reduced = parts.astype(F32).sum(axis=0).astype(BF16)
    return (hidden.astype(F32) + sum_over_groups(reduced)).astype(BF16)


def solution(mesh):
    split = Mesh(
        mesh.devices.reshape(mesh.shape["expert"], 4, 4, 2),
        ("expert", "shard_0", "shard_1", "shard_2"),
    )
    in_specs = (
        P(SHARD, None),
        P(SHARD, "expert", None),
        P(SHARD, None, "expert", None),
        P(SHARD, None, "expert", None),
        P("expert", SHARD),
        P(),
        P(),
        P(),
        P("expert", None, SHARD),
        P("expert", None, SHARD),
        P("expert", SHARD, None),
    )
    return jax.shard_map(
        on_device, mesh=split, in_specs=in_specs, out_specs=P(SHARD, None), check_vma=False
    )
```

```python
import math

import jax
import jax.numpy as jnp
from jax import lax
from jax.experimental import pallas as pl
from jax.experimental.pallas import tpu as pltpu
from jax.sharding import Mesh
from jax.sharding import PartitionSpec as P

SHARD = ("shard_0", "shard_1", "shard_2")
PLANE = ("shard_0", "shard_1")
F32 = jnp.float32
BF16 = jnp.bfloat16
BRING_GRANT = 40 * 1024 * 1024
EXPERT_GRANT = 36 * 1024 * 1024


def shifted(x, axis, by):
    size = lax.axis_size(axis)
    return lax.ppermute(x, axis, [(i, (i + by) % size) for i in range(size)])


def sum_over_groups(part, ready=()):
    others = tuple(shifted(part, "expert", by) for by in (1, 2, 3))
    (one, two, three), ready = lax.optimization_barrier((others, ready))
    total = (part.astype(F32) + two.astype(F32)) + (one.astype(F32) + three.astype(F32))
    return (total, ready) if ready else total


def attention_kernel(queries, hidden, key_hbm, value_hbm, pieces, keys, values, scores, found, sems):
    tokens, rows, size = keys.shape
    heads = queries.shape[0] // tokens
    kv_local = 2
    parts = sems.shape[1]
    count = tokens // parts

    def copy(n, part):
        source, target = ((key_hbm, keys), (value_hbm, values))[n]
        at = pl.ds(part * count, count)
        return pltpu.make_async_copy(source.at[at], target.at[at], sems.at[n, part])

    for n in range(2):
        for part in range(parts):
            copy(n, part).start()

    def score_part(part, carry):
        copy(0, part).wait()
        for m in range(count):
            t = part * count + m
            at = pl.ds(pl.multiple_of(t * heads, heads), heads)
            scores[at, :] = lax.dot_general(
                queries[at, :], keys[t], (((1,), (1,)), ((), ())), preferred_element_type=F32
            )
        return carry

    lax.fori_loop(0, parts, score_part, 0)
    chips, _, columns = pieces.shape
    block = columns - heads * size
    for chip in range(chips):
        pieces[chip, :, heads * size :] = hidden[:, chip * block : (chip + 1) * block]
    shape = scores.shape
    mine = (lax.broadcasted_iota(jnp.int32, shape, 0) % heads) // (heads // kv_local) == (
        lax.broadcasted_iota(jnp.int32, shape, 1) % kv_local
    )
    logits = jnp.where(mine, scores[...] * (1.0 / math.sqrt(size)), -3.0e38)
    powers = jnp.exp(logits - logits.max(axis=1, keepdims=True))
    scores[...] = powers / powers.sum(axis=1, keepdims=True)

    def wait_part(part, carry):
        copy(1, part).wait()
        return carry

    lax.fori_loop(0, parts, wait_part, 0)
    for t in range(tokens):
        at = pl.ds(t * heads, heads)
        found[at, :] = jnp.dot(
            scores[at, :].astype(BF16), values[t], preferred_element_type=F32
        )
    for h in range(heads):
        attended = found[pl.ds(h, tokens, stride=heads), :].astype(BF16)
        for chip in range(chips):
            pieces[chip, :, h * size : (h + 1) * size] = attended


def attention(queries, keys, values, hidden, chips):
    tokens, heads, size = queries.shape
    rows = keys.shape[1]
    width = heads * size + hidden.shape[1] // chips
    vmem = pl.BlockSpec(memory_space=pltpu.VMEM)
    hbm = pl.BlockSpec(memory_space=pl.ANY)
    return pl.pallas_call(
        attention_kernel,
        out_shape=jax.ShapeDtypeStruct((chips, tokens, width), BF16),
        in_specs=[vmem, vmem, hbm, hbm],
        out_specs=vmem,
        scratch_shapes=[
            pltpu.VMEM((tokens, rows, size), BF16),
            pltpu.VMEM((tokens, rows, size), BF16),
            pltpu.VMEM((tokens * heads, rows), F32),
            pltpu.VMEM((tokens * heads, size), F32),
            pltpu.SemaphoreType.DMA((2, 4)),
        ],
        compiler_params=pltpu.CompilerParams(vmem_limit_bytes=62 * 1024 * 1024),
        cost_estimate=pl.CostEstimate(
            flops=4 * tokens * heads * rows * size,
            bytes_accessed=4 * tokens * rows * size,
            transcendentals=tokens * heads * rows,
        ),
        name="attention",
    )(queries.reshape(tokens * heads, size), hidden, keys, values)


def spread_kernel(_, gains, gain):
    lanes = gain.shape[1]
    for at in range(0, gain.shape[0], lanes):
        row = gains[:, at : at + lanes].astype(F32)
        gain[at : at + lanes, :] = jnp.broadcast_to(row, (lanes, lanes)).T.astype(BF16)


def spread(after, gains):
    size = gains.shape[1]
    vmem = pl.BlockSpec(memory_space=pltpu.VMEM)
    return pl.pallas_call(
        spread_kernel,
        out_shape=jax.ShapeDtypeStruct((size, 128), BF16),
        in_specs=[pl.BlockSpec(memory_space=pl.ANY), vmem],
        out_specs=vmem,
        compiler_params=pltpu.CompilerParams(vmem_limit_bytes=4 * 1024 * 1024),
        cost_estimate=pl.CostEstimate(
            flops=20000 * size, bytes_accessed=256 * size, transcendentals=0
        ),
        name="spread",
    )(after, gains)


def bring_kernel(_, source, target, sem):
    copy = pltpu.make_async_copy(source, target, sem)
    copy.start()
    copy.wait()


def brought_in(after, weights):
    hbm = pl.BlockSpec(memory_space=pl.ANY)
    return pl.pallas_call(
        bring_kernel,
        out_shape=pltpu.VMEM(weights.shape, weights.dtype),
        in_specs=[hbm, hbm],
        out_specs=pl.BlockSpec(memory_space=pltpu.VMEM),
        scratch_shapes=[pltpu.SemaphoreType.DMA],
        compiler_params=pltpu.CompilerParams(vmem_limit_bytes=BRING_GRANT),
        cost_estimate=pl.CostEstimate(
            flops=80 * weights.size, bytes_accessed=4 * weights.size, transcendentals=0
        ),
        name="bring",
    )(after, weights)


def expert_kernel(
    place, ids, gain, router, attn, gate, own, partner, up_hbm, down_hbm,
    send, keep, mixed, hidden_t, act, up, down, sems,
):
    core, shard, first_expert, adds = (place[n] for n in range(4))
    units, width = gate.shape
    half_units = units // 2
    chips, block, tokens = own.shape
    half = tokens // 2
    step = width // 2

    def up_copy(m):
        rows = pl.ds(pl.multiple_of(m * half_units, half_units), half_units)
        return pltpu.make_async_copy(up_hbm.at[rows], up.at[rows], sems.at[m])

    def down_copy(n):
        columns = pl.ds(pl.multiple_of(n * step, step), step)
        return pltpu.make_async_copy(
            down_hbm.at[:, columns], down.at[:, columns], sems.at[2 + n]
        )

    for m in range(2):
        up_copy(m).start()
    for n in range(2):
        down_copy(n).start()

    def norm_block(j, squares):
        for mine, part in ((core, own), (1 - core, partner)):
            x = part[j]
            if part is partner:
                x = jnp.concatenate([x[:, half:], x[:, :half]], axis=1)
            rows = pl.ds(pl.multiple_of((2 * j + mine) * block, block), block)
            g = gain[rows, :]
            mixed[rows, :] = x * jnp.concatenate([g, g], axis=1)
            y = x.astype(F32)
            squares = squares + (y * y).reshape(block // 8, 8, tokens).sum(axis=0)
        return squares

    squares = lax.fori_loop(0, chips, norm_block, jnp.zeros((8, tokens), F32), unroll=4)
    scale = lax.rsqrt(squares.sum(axis=0, keepdims=True) / width + 1e-05)
    logits = jnp.dot(router[...], mixed[...], preferred_element_type=F32) * scale
    numbers = lax.broadcasted_iota(jnp.int32, logits.shape, 0)
    named = ids[...]
    named = jnp.where(
        core == 0, named, jnp.concatenate([named[:, half:], named[:, :half]], axis=1)
    )
    first, second = named[0:1, :], named[1:2, :]
    a = jnp.where(numbers == first, logits, 0.0).sum(axis=0, keepdims=True)
    b = jnp.where(numbers == second, logits, 0.0).sum(axis=0, keepdims=True)
    weight_first = 1.0 / (1.0 + jnp.exp(b - a))
    weight_second = 1.0 / (1.0 + jnp.exp(a - b))

    for m in range(2):
        rows = pl.ds(m * half_units, half_units)
        hidden_t[0, m] = jnp.dot(gate[rows, :], mixed[...], preferred_element_type=F32)

    def up_part(m, carry):
        up_copy(m).wait()
        rows = pl.ds(pl.multiple_of(m * half_units, half_units), half_units)
        hidden_t[1, m] = jnp.dot(up[rows, :], mixed[...], preferred_element_type=F32)
        return carry

    lax.fori_loop(0, 2, up_part, 0)
    for m in range(2):
        expert = first_expert + m
        routed = jnp.where(first == expert, weight_first, 0.0) + jnp.where(
            second == expert, weight_second, 0.0
        )
        gated = hidden_t[0, m] * scale
        upward = hidden_t[1, m] * scale
        value = gated / (1.0 + jnp.exp(-gated)) * upward * routed
        act[m] = value.T.astype(BF16)

    def down_part(n, carry):
        down_copy(n).wait()
        columns = pl.ds(pl.multiple_of(n * step, step), step)
        total = jnp.dot(
            act[0], down[pl.ds(0, half_units), columns], preferred_element_type=F32
        ) + jnp.dot(
            act[1], down[pl.ds(half_units, half_units), columns], preferred_element_type=F32
        )
        keep[:, columns] = total[:half].astype(BF16)
        send[:, columns] = total[half:].astype(BF16)
        return carry

    lax.fori_loop(0, 2, down_part, 0)
    rows = attn[...].astype(F32).T * adds.astype(F32)
    columns = pl.ds(pl.multiple_of(shard * block, block), block)
    keep[:, columns] = (keep[:, columns].astype(F32) + rows[:half]).astype(BF16)
    send[:, columns] = (send[:, columns].astype(F32) + rows[half:]).astype(BF16)


def experts(place, ids, gain, router, attn, gate, own, partner, up, down):
    units, width = gate.shape
    tokens = attn.shape[1]
    vmem = pl.BlockSpec(memory_space=pltpu.VMEM)
    hbm = pl.BlockSpec(memory_space=pl.ANY)
    half = jax.ShapeDtypeStruct((tokens // 2, width), BF16)
    return pl.pallas_call(
        expert_kernel,
        out_shape=(half, half),
        in_specs=[pl.BlockSpec(memory_space=pltpu.SMEM)] + [vmem] * 7 + [hbm] * 2,
        out_specs=(vmem, vmem),
        scratch_shapes=[
            pltpu.VMEM((width, tokens), BF16),
            pltpu.VMEM((2, 2, units // 2, tokens), F32),
            pltpu.VMEM((2, tokens, units // 2), BF16),
            pltpu.VMEM((units, width), BF16),
            pltpu.VMEM((units, width), BF16),
            pltpu.SemaphoreType.DMA((4,)),
        ],
        compiler_params=pltpu.CompilerParams(vmem_limit_bytes=EXPERT_GRANT),
        cost_estimate=pl.CostEstimate(
            flops=6 * tokens * units * width,
            bytes_accessed=6 * units * width,
            transcendentals=2 * units * tokens,
        ),
        name="experts",
    )(place, ids, gain, router, attn, gate, own, partner, up, down)


def on_device(
    hidden, queries, key_cache, value_cache, out_weight, norm_gain, router,
    expert_ids, gate_weight, up_weight, down_weight,
):
    count_local, heads_local, head_size = queries.shape
    kv_local = key_cache.shape[2]
    width = hidden.shape[1]
    block = out_weight.shape[1]
    chips, cores = lax.axis_size(PLANE), lax.axis_size("shard_2")
    tokens = chips * cores * count_local
    core = lax.axis_index("shard_2")
    group = lax.axis_index("expert")
    heads = heads_local * head_size
    rows = key_cache.shape[1] * kv_local
    pieces = attention(
        queries,
        key_cache.reshape(count_local, rows, head_size),
        value_cache.reshape(count_local, rows, head_size),
        hidden,
        chips,
    )
    local = gate_weight.shape[0]
    units = local * gate_weight.shape[2]
    place = jnp.stack(
        [
            core,
            lax.axis_index(PLANE) * cores + core,
            group * local,
            (group == 0).astype(jnp.int32),
        ]
    ).astype(jnp.int32)
    ids = expert_ids.reshape(chips, cores, count_local, 2).transpose(3, 1, 0, 2).reshape(2, tokens)
    arrived = lax.all_to_all(pieces, PLANE, 0, 0, tiled=True).reshape(tokens // 2, -1)
    arrived, place, ids = lax.optimization_barrier((arrived, place, ids))
    passed = shifted(arrived, "shard_2", 1)

    def project(rows):
        return lax.dot_general(
            out_weight, rows[:, :heads], (((0,), (1,)), ((), ())), preferred_element_type=F32
        ).astype(BF16)

    def my_columns(rows):
        return jnp.where(core == 0, rows[:, heads : heads + block], rows[:, heads + block :])

    part = jnp.concatenate([project(arrived), project(passed)], axis=1)
    hidden_t = jnp.concatenate([my_columns(arrived), my_columns(passed)], axis=0).T
    gain = spread(part, norm_gain[None, :])
    gate = brought_in(part, gate_weight.transpose(0, 2, 1).reshape(units, width))
    attn_out, (hidden_t, gain, gate) = sum_over_groups(part, (hidden_t, gain, gate))
    stream = (attn_out + hidden_t.astype(F32)).astype(BF16)
    own = lax.all_to_all(
        jnp.broadcast_to(stream[None], (chips, block, tokens)), PLANE, 0, 0, tiled=True
    )
    partner = shifted(own, "shard_2", 1)
    send, keep = experts(
        place,
        ids,
        gain,
        router.T,
        attn_out.astype(BF16),
        gate,
        own,
        partner,
        up_weight.transpose(0, 2, 1).reshape(units, width),
        down_weight.reshape(units, width),
    )
    pair = (keep.astype(F32) + shifted(send, "shard_2", 1).astype(F32)).astype(BF16)
    parts = lax.all_to_all(pair.reshape(chips, count_local, width), PLANE, 0, 0, tiled=True)
    reduced = parts.astype(F32).sum(axis=0).astype(BF16)
    return (hidden.astype(F32) + sum_over_groups(reduced)).astype(BF16)


def solution(mesh):
    split = Mesh(
        mesh.devices.reshape(mesh.shape["expert"], 4, 4, 2),
        ("expert", "shard_0", "shard_1", "shard_2"),
    )
    in_specs = (
        P(SHARD, None),
        P(SHARD, "expert", None),
        P(SHARD, None, "expert", None),
        P(SHARD, None, "expert", None),
        P("expert", SHARD),
        P(),
        P(),
        P(),
        P("expert", None, SHARD),
        P("expert", None, SHARD),
        P("expert", SHARD, None),
    )
    return jax.shard_map(
        on_device, mesh=split, in_specs=in_specs, out_specs=P(SHARD, None), check_vma=False
    )
```
